256 devices in a mesh: blk: 16 (over z, core), section: 16 (over y, x).
Axes of the slice: x: 4, y: 4, z: 8, core: 2. Of those that a mesh axis runs over, the one named last changes fastest.
Arguments:
- hidden: bfloat16 [16, 2048, 2048], P('section', 'blk'), parts along dimension 1, may hold values from -6 to 6
- exit_layer: int32 [8192], P('blk'), parts along dimension 0, may hold values from 1 to 4
- lengths: int32 [8192], P('blk'), parts along dimension 0, may hold values from 1 to 16, as said below
- kv_cache: bfloat16 [16, 2048, 16, 256], P('section', 'blk'), parts along dimension 1, may hold values from -256 to 256
- norm_gain: bfloat16 [16, 2048], P('section'), may hold values from 0.5 to 1.5
- w_qkv: bfloat16 [16, 2048, 1280], P('section'), may hold values from -0.0625 to 0.0625
- w_out: bfloat16 [16, 1024, 2048], P('section'), may hold values from -0.1875 to 0.1875
Outputs:
- settled: bfloat16 [8192, 8192], P('blk', 'section'), parts along dimension 0
The draws below stay inside these ranges and needn't reach their ends.
There are 16 independent parts, one for each index of `blk`. The reference program is written for one: setup_inputs(seed, part) draws one part's arguments, and reference() takes and returns one part's arrays. A program takes and returns all parts, laid end to end along the dimension named above; an argument that names none is the same for every part. Nothing has to cross between parts.
Inputs may be any that keep to these rules, and one draw needn't show every extreme that they name: `lengths`: some token has length 16.
All inputs are finite; a program needn't handle non-finite values.
Results may differ from the reference program's by a relative error of at most 0.03.
Values may be sent and summed in bfloat16 or wider, within the bound.
A program may use at most 64 MiB of HBM per device.

```python
import jax
import jax.numpy as jnp
from jax import lax

D = 8192
HD = 128
QH = 8
BLOCK = 64
MICRO = 8
CTX = 16
SHARDS = 4
LAYERS = 4
TOKENS = 512


def draw_exit_layer(key, part):
    count_key = jax.random.fold_in(key, 11)
    order_key = jax.random.fold_in(key, 13)
    depth_key = jax.random.fold_in(key, 14)
    counts = jax.random.randint(count_key, (MICRO,), BLOCK // 4, BLOCK // 2 + 1)
    scores = jax.random.randint(order_key, (MICRO, BLOCK), 0, 1 << 20) * BLOCK + jnp.arange(BLOCK)[None, :]
    ranking = jnp.argsort(jnp.argsort(scores, axis=1), axis=1)
    deeper = ranking < counts[:, None]
    depth = jax.random.randint(depth_key, (MICRO, BLOCK), 2, LAYERS + 1)
    return jnp.where(deeper, depth, 1).reshape(-1).astype(jnp.int32)


def draw_lengths(key, part):
    length_key = jax.random.fold_in(key, 21)
    forced_key = jax.random.fold_in(key, 22)
    drawn = jax.random.randint(length_key, (TOKENS,), 1, CTX + 1)
    forced = jax.random.randint(forced_key, (), 0, TOKENS)
    return jnp.where(jnp.arange(TOKENS) == forced, CTX, drawn).astype(jnp.int32)


def draw_kv_cache(key, part):
    keys_key = jax.random.fold_in(key, 31)
    values_key = jax.random.fold_in(key, 32)
    shape = (SHARDS * LAYERS, TOKENS // SHARDS, CTX, HD)
    keys = jax.random.truncated_normal(keys_key, -4.0, 4.0, shape, jnp.float32)
    values = jax.random.truncated_normal(values_key, -4.0, 4.0, shape, jnp.float32)
    return jnp.concatenate([keys, values], axis=-1).astype(jnp.bfloat16)


def steps_of(key, dims, cuts, low, largest):
    def one(dim, shards_of):
        draws = jax.random.uniform(jax.random.fold_in(jax.random.fold_in(key, 6), dim), (shards_of,), jnp.float32, low / len(cuts), largest / len(cuts))
        return jnp.repeat(jnp.exp(draws), dims[dim] // shards_of).reshape((-1,) + (1,) * (len(dims) - dim - 1))

    loudness = one(*cuts[0])
    for cut in cuts[1:]:
        loudness = loudness * one(*cut)
    return loudness


def centred(stream_key, extent, spread, limit, shards=(), held_as=jnp.bfloat16):
    values = spread * jax.random.normal(stream_key, extent, jnp.float32)
    if shards:
        values = values * steps_of(stream_key, extent, shards, -0.22, 0.18)
    return jnp.clip(values, -limit, limit).astype(held_as)


def setup_inputs(seed: int = 0, part: int = 0) -> dict:
    arg_keys = jax.random.split(jax.random.key(seed), 8)
    own_keys = jax.random.split(jax.random.fold_in(arg_keys[7], part), 8)
    hidden = centred(own_keys[0], (SHARDS * LAYERS, TOKENS // LAYERS, D // SHARDS), 1.0, 6.0, ((0, 16),))
    exit_layer = draw_exit_layer(jax.random.fold_in(jax.random.fold_in(arg_keys[7], part), 71), part)
    lengths = draw_lengths(jax.random.fold_in(jax.random.fold_in(arg_keys[7], part), 71), part)
    kv_cache = draw_kv_cache(jax.random.fold_in(jax.random.fold_in(arg_keys[7], part), 71), part)
    norm_gain = jnp.clip(1.0 + 0.1 * jax.random.normal(arg_keys[4], (SHARDS * LAYERS, D // SHARDS), jnp.float32), 0.5, 1.5).astype(jnp.bfloat16)
    w_qkv = centred(arg_keys[5], (SHARDS * LAYERS, D // SHARDS, (QH + 2) * HD), D ** -0.5, 0.0625, ((0, 16),))
    w_out = centred(arg_keys[6], (SHARDS * LAYERS, QH * HD, D // SHARDS), (QH * HD) ** -0.5, 0.1875, ((0, 16),))
    return dict(hidden=hidden, exit_layer=exit_layer, lengths=lengths, kv_cache=kv_cache, norm_gain=norm_gain, w_qkv=w_qkv, w_out=w_out)


EPSILON = 1e-05
NEGATIVE = -1e+30

def attend(state, active, len_rows, cache_rows, gain_row, proj_weight, out_weight):
    query_width = out_weight.shape[0]
    head_size = (proj_weight.shape[1] - query_width) // 2
    heads = query_width // head_size
    rows = state.shape[0]
    context = cache_rows.shape[1]
    widened = state.astype(jnp.float32)
    scaled = (widened * gain_row.astype(jnp.float32)).astype(jnp.bfloat16)
    mean_square = lax.optimization_barrier(jnp.mean(widened * widened, axis=-1))
    projected = jnp.dot(scaled, proj_weight, preferred_element_type=jnp.float32) * lax.rsqrt(mean_square + EPSILON)[:, None]
    query = (projected[:, :query_width] * (1.0 / jnp.sqrt(jnp.float32(head_size)))).astype(jnp.bfloat16)
    query = query.reshape(rows, heads, head_size).astype(jnp.float32)
    key_new = projected[:, query_width:query_width + head_size].astype(jnp.bfloat16).astype(jnp.float32)
    value_new = projected[:, query_width + head_size:].astype(jnp.bfloat16).astype(jnp.float32)
    keys = cache_rows[:, :, :head_size].astype(jnp.float32)
    values = cache_rows[:, :, head_size:].astype(jnp.float32)
    scores = jnp.einsum('rhd,rcd->rhc', query, keys)
    own = jnp.einsum('rhd,rd->rh', query, key_new)
    positions = jnp.arange(context, dtype=jnp.int32)
    usable = (positions[None, :] < len_rows[:, None])[:, None, :]
    scores = jnp.where(usable, scores, NEGATIVE)
    row_top = jnp.maximum(lax.optimization_barrier(jnp.max(scores, axis=-1)), own)
    raw = jnp.where(usable, jnp.exp(scores - row_top[:, :, None]), jnp.float32(0.0))
    raw_own = jnp.exp(own - row_top)
    total = lax.optimization_barrier(jnp.sum(raw, axis=-1)) + raw_own
    weights = (raw / total[:, :, None]).astype(jnp.bfloat16).astype(jnp.float32)
    own_weight = (raw_own / total).astype(jnp.bfloat16).astype(jnp.float32)
    attended = jnp.einsum('rhc,rcd->rhd', weights, values) + own_weight[:, :, None] * value_new[:, None, :]
    attended = attended.astype(jnp.bfloat16).reshape(rows, query_width)
    branch_out = jnp.dot(attended, out_weight, preferred_element_type=jnp.float32)
    updated = (widened + branch_out).astype(jnp.bfloat16)
    return jnp.where(active[:, None], updated, state)

def reference(hidden, exit_layer, lengths, kv_cache, norm_gain, w_qkv, w_out):
    group = BLOCK // SHARDS
    span = D // (SHARDS * LAYERS)
    columns = w_qkv.shape[2]
    query_width = w_out.shape[1]
    width = kv_cache.shape[3]
    rounds = MICRO // LAYERS
    gains = norm_gain.reshape(LAYERS, SHARDS, LAYERS, span).transpose(0, 2, 1, 3).reshape(LAYERS, D)
    projections = w_qkv.reshape(LAYERS, SHARDS, LAYERS, span, columns).transpose(0, 2, 1, 3, 4).reshape(LAYERS, D, columns)
    outputs = w_out.reshape(LAYERS, SHARDS, query_width, LAYERS, span).transpose(0, 2, 3, 1, 4).reshape(LAYERS, query_width, D)
    cache = kv_cache.reshape(LAYERS, SHARDS, MICRO, group, CTX, width).transpose(0, 2, 1, 3, 4, 5).reshape(LAYERS, MICRO * BLOCK, CTX, width)
    arranged = hidden.reshape(LAYERS, SHARDS, rounds, BLOCK, LAYERS, span).transpose(2, 0, 3, 4, 1, 5).reshape(rounds, LAYERS, BLOCK, D)
    arranged = jnp.stack([arranged[:, (LAYERS - place) % LAYERS] for place in range(LAYERS)], axis=1)
    state = arranged.reshape(MICRO * BLOCK, D)
    for layer in range(LAYERS):
        state = attend(state, exit_layer > layer, lengths, cache[layer], gains[layer], projections[layer], outputs[layer])
    return state
```

```python
import functools
import math

import jax
import jax.numpy as jnp
from jax import lax
from jax.experimental import pallas as pl
from jax.experimental.pallas import tpu as pltpu
from jax.sharding import PartitionSpec as P

BLOCK = 64
MICRO = 8
EPSILON = 1e-05
NEGATIVE = -1e30
TAIL = 128
MESH = pl.DeviceIdType.MESH
F32 = jnp.float32
BF16 = jnp.bfloat16


def kernel(
    shards,
    layers,
    hidden,
    gain,
    wq_hbm,
    wo_hbm,
    cache_hbm,
    exits,
    lens,
    out,
    wq,
    wo,
    cache,
    inb,
    outb,
    accs,
    rs_send,
    rs_recv,
    att,
    w_sem,
    hid_ss,
    in_rs,
    rs_ss,
    rs_rs,
    ag_ss,
    ag_rs,
    st_ss,
    out_rs,
):
    me = lax.axis_index("section")
    y = me // shards
    x = me % shards
    last = layers - 1
    span = inb.shape[3]
    group = BLOCK // shards
    query_width = wo.shape[1]
    width = wq.shape[2]
    head = (width - query_width) // 2
    heads = query_width // head
    context = cache.shape[0] // (MICRO * group)
    total_width = span * shards * layers

    def remote(src, dst, send_sem, recv_sem, target):
        return pltpu.make_async_remote_copy(
            src_ref=src,
            dst_ref=dst,
            send_sem=send_sem,
            recv_sem=recv_sem,
            device_id={"section": target},
            device_id_type=MESH,
        )

    def row_peer(d):
        return y * shards + (x + d) % shards

    wq_copies = [
        pltpu.make_async_copy(wq_hbm.at[pl.ds(j * span, span)], wq.at[j], w_sem.at[j])
        for j in range(layers)
    ]
    wo_copies = [
        pltpu.make_async_copy(
            wo_hbm.at[:, pl.ds(j * span, span)], wo.at[j], w_sem.at[layers + j]
        )
        for j in range(layers)
    ]
    cache_copy = pltpu.make_async_copy(cache_hbm, cache, w_sem.at[2 * layers])
    for copy in wq_copies:
        copy.start()
    cache_copy.start()
    for copy in wo_copies:
        copy.start()

    barrier = pltpu.get_barrier_semaphore()
    for d in range(1, shards):
        pl.semaphore_signal(
            barrier, inc=1, device_id={"section": row_peer(d)}, device_id_type=MESH
        )
    for d in range(1, layers):
        pl.semaphore_signal(
            barrier,
            inc=1,
            device_id={"section": ((y + d) % layers) * shards + x},
            device_id_type=MESH,
        )
    pl.semaphore_wait(barrier, shards + layers - 2)

    rounds = MICRO // layers
    place = (layers - y) % layers

    def hidden_piece(q, j):
        return hidden.at[pl.ds(q * BLOCK, BLOCK), pl.ds(j * span, span)]

    def hidden_copy(q, j):
        m = q * layers + place
        return remote(
            hidden_piece(q, j), inb.at[m, j], hid_ss.at[q, j], in_rs.at[m, j], x
        )

    @pl.when(y == 0)
    def _():
        for q in range(rounds):
            for j in range(layers):
                pltpu.make_async_copy(
                    hidden_piece(q, j), inb.at[q * layers, j], in_rs.at[q * layers, j]
                ).start()

    @pl.when(y != 0)
    def _():
        for q in range(rounds):
            for j in range(layers):
                hidden_copy(q, j).start()

    def rs_copy(i, d):
        target = (x + d) % shards
        return remote(
            rs_send.at[i, target],
            rs_recv.at[i, x],
            rs_ss.at[i, d - 1],
            rs_rs.at[i, x],
            row_peer(d),
        )

    def rs_arrival(i, d):
        source = (x + d) % shards
        return remote(
            rs_send.at[i, source],
            rs_recv.at[i, source],
            rs_ss.at[i, d - 1],
            rs_rs.at[i, source],
            row_peer(d),
        )

    def ag_copy(i, d):
        return remote(
            att.at[i, x], att.at[i, x], ag_ss.at[i, d - 1], ag_rs.at[i, x], row_peer(d)
        )

    def ag_arrival(i, d):
        source = (x + d) % shards
        return remote(
            att.at[i, source],
            att.at[i, source],
            ag_ss.at[i, d - 1],
            ag_rs.at[i, source],
            row_peer(d),
        )

    def state_copy(i, j):
        return remote(
            outb.at[i, j],
            inb.at[i, j],
            st_ss.at[i, j],
            in_rs.at[i, j],
            (me + shards) % (shards * layers),
        )

    def out_rows(i):
        return pl.ds(pl.multiple_of(i * BLOCK, BLOCK), BLOCK)

    def result_copy(i, j):
        return remote(
            outb.at[i, j], out.at[out_rows(i)], st_ss.at[i, j], out_rs.at[i], j * shards + x
        )

    def project(i):
        squares = jnp.zeros((BLOCK, TAIL), F32)
        acc = None
        for j in range(layers):

            @pl.when(i == 0)
            def _():
                wq_copies[j].wait()

            state_copy(i, j).wait_recv()
            state = inb[i, j].astype(F32)
            scaled = (state * gain[:, pl.ds(j * span, span)].astype(F32)).astype(BF16)
            squared = state * state
            for n in range(span // TAIL):
                squares = squares + squared[:, n * TAIL : (n + 1) * TAIL]
            part = jnp.dot(scaled, wq[j], preferred_element_type=F32)
            acc = part if acc is None else acc + part
        total = jnp.sum(squares, axis=1, keepdims=True)
        coarse = total.astype(BF16).astype(F32)
        lane = lax.broadcasted_iota(jnp.int32, (BLOCK, TAIL), 1)
        tail = jnp.where(lane < TAIL // 2, coarse, total - coarse)
        accs[:, :width] = acc
        accs[:, width:] = tail
        narrow = acc.astype(BF16)
        narrow_tail = tail.astype(BF16)
        for g in range(shards):
            rs_send[i, g, :, :width] = narrow[g * group : (g + 1) * group]
            rs_send[i, g, :, width:] = narrow_tail[g * group : (g + 1) * group]
        for d in (2, 1, 3):
            rs_copy(i, d).start()

    def attend(i):
        @pl.when(i == 0)
        def _():
            cache_copy.wait()

        summed = accs[pl.ds(pl.multiple_of(x * group, group), group), :]
        for d in (1, 3, 2):
            rs_arrival(i, d).wait_recv()
        for d in (1, 3, 2):
            summed = summed + rs_recv[i, (x + d) % shards].astype(F32)
        squares = jnp.sum(summed[:, width:], axis=1, keepdims=True) * (2.0 / TAIL)
        scale = lax.rsqrt(squares / total_width + EPSILON)
        fitted = summed[:, :width] * scale
        query = (fitted[:, :query_width] * (1.0 / math.sqrt(head))).astype(BF16)
        query = jnp.concatenate(
            [query[:, h * head : (h + 1) * head] for h in range(heads)], axis=0
        )
        key_new = fitted[:, query_width : query_width + head].astype(BF16).astype(F32)
        value_new = fitted[:, query_width + head :].astype(BF16).astype(F32)
        key_new = jnp.concatenate([key_new] * heads, axis=0)
        value_new = jnp.concatenate([value_new] * heads, axis=0)
        rows = pl.ds(pl.multiple_of(i * (group * context), group * context), group * context)
        keys = cache[rows, :head]
        values = cache[rows, head:]
        scores = lax.dot_general(
            query, keys, (((1,), (1,)), ((), ())), preferred_element_type=F32
        )
        own = jnp.sum(query.astype(F32) * key_new, axis=1, keepdims=True)
        span_of = lens[pl.ds(pl.multiple_of(i * BLOCK + x * group, group), group), :]
        span_of = jnp.concatenate([span_of] * (group * context // TAIL), axis=1)
        span_of = jnp.concatenate([span_of] * heads, axis=0)
        shape = (heads * group, group * context)
        row = lax.broadcasted_iota(jnp.int32, shape, 0)
        column = lax.broadcasted_iota(jnp.int32, shape, 1)
        offset = column - (row % group) * context
        usable = (offset >= 0) & (offset < span_of)
        scores = jnp.where(usable, scores, NEGATIVE)
        top = jnp.maximum(jnp.max(scores, axis=1, keepdims=True), own)
        raw = jnp.where(usable, jnp.exp(scores - top), 0.0)
        raw_own = jnp.exp(own - top)
        total = jnp.sum(raw, axis=1, keepdims=True) + raw_own
        inverse = 1.0 / total
        weights = (raw * inverse).astype(BF16)
        own_weight = (raw_own * inverse).astype(BF16).astype(F32)
        attended = jnp.dot(weights, values, preferred_element_type=F32)
        attended = (attended + own_weight * value_new).astype(BF16)
        att[i, x] = jnp.concatenate(
            [attended[h * group : (h + 1) * group] for h in range(heads)], axis=1
        )
        for d in (2, 1, 3):
            ag_copy(i, d).start()

    def update(i):
        for d in (1, 3, 2):
            ag_arrival(i, d).wait_recv()
        attended = att[i].reshape(BLOCK, query_width)
        depth = exits[out_rows(i), :]
        active = jnp.concatenate([depth] * (span // TAIL), axis=1) > y
        for j in range(layers):

            @pl.when(i == 0)
            def _():
                wo_copies[j].wait()

            state = inb[i, j].astype(F32)
            branch = jnp.dot(attended, wo[j], preferred_element_type=F32)
            updated = jnp.where(active, state + branch, state).astype(BF16)
            outb[i, j] = updated

            @pl.when(y < last)
            def _():
                state_copy(i, j).start()

            if j < last:

                @pl.when(y == last)
                def _():
                    result_copy(i, j).start()

            else:

                @pl.when(y == last)
                def _():
                    out[out_rows(i), :] = updated

    def step(i, carry):
        @pl.when(i < MICRO)
        def _():
            project(i)

        @pl.when(i > 0)
        def _():
            update(i - 1)

        @pl.when(i < MICRO)
        def _():
            attend(i)

        return carry

    lax.fori_loop(0, MICRO + 1, step, 0)

    def finish(i, carry):
        for d in range(1, shards):
            rs_copy(i, d).wait_send()
            ag_copy(i, d).wait_send()
        for j in range(layers):

            @pl.when(y < last)
            def _():
                state_copy(i, j).wait_send()

            if j < last:

                @pl.when(y == last)
                def _():
                    result_copy(i, j).wait_send()

        @pl.when(y < last)
        def _():
            result_copy(i, 0).wait_recv()

        return carry

    lax.fori_loop(0, MICRO, finish, 0)

    @pl.when(y != 0)
    def _():
        for q in range(rounds):
            for j in range(layers):
                hidden_copy(q, j).wait_send()


def body(hidden, exit_layer, lengths, kv_cache, norm_gain, w_qkv, w_out):
    devices = lax.axis_size("section")
    shards = max(2, devices // 4)
    layers = devices // shards
    own_hidden = hidden[0]
    proj_weight = w_qkv[0]
    out_weight = w_out[0]
    tokens = exit_layer.shape[0]
    quarter, width = proj_weight.shape
    query_width = out_weight.shape[0]
    span = quarter // layers
    group = BLOCK // shards
    cache_rows = kv_cache.shape[1] * kv_cache.shape[2]
    cache = kv_cache.reshape(cache_rows, kv_cache.shape[3])
    exits = jnp.broadcast_to(exit_layer[:, None], (tokens, TAIL))
    lens = jnp.broadcast_to(lengths[:, None], (tokens, TAIL))
    anywhere = pl.BlockSpec(memory_space=pl.ANY)
    vmem = pl.BlockSpec(memory_space=pltpu.VMEM)
    dma = pltpu.SemaphoreType.DMA
    return pl.pallas_call(
        functools.partial(kernel, shards, layers),
        out_shape=jax.ShapeDtypeStruct((tokens, span), BF16),
        in_specs=[anywhere, vmem, anywhere, anywhere, anywhere, vmem, vmem],
        out_specs=vmem,
        scratch_shapes=[
            pltpu.VMEM((layers, span, width), BF16),
            pltpu.VMEM((layers, query_width, span), BF16),
            pltpu.VMEM(cache.shape, BF16),
            pltpu.VMEM((MICRO, layers, BLOCK, span), BF16),
            pltpu.VMEM((MICRO, layers, BLOCK, span), BF16),
            pltpu.VMEM((BLOCK, width + TAIL), F32),
            pltpu.VMEM((MICRO, shards, group, width + TAIL), BF16),
            pltpu.VMEM((MICRO, shards, group, width + TAIL), BF16),
            pltpu.VMEM((MICRO, shards, group, query_width), BF16),
            dma((2 * layers + 1,)),
            dma((MICRO // layers, layers)),
            dma((MICRO, layers)),
            dma((MICRO, shards - 1)),
            dma((MICRO, shards)),
            dma((MICRO, shards - 1)),
            dma((MICRO, shards)),
            dma((MICRO, layers)),
            dma((MICRO,)),
        ],
        compiler_params=pltpu.CompilerParams(
            collective_id=0, has_side_effects=True, vmem_limit_bytes=56 << 20
        ),
    )(own_hidden, norm_gain, proj_weight, out_weight, cache, exits, lens)


def solution(mesh):
    return jax.shard_map(
        body,
        mesh=mesh,
        in_specs=(
            P("section", "blk", None),
            P("blk"),
            P("blk"),
            P("section", "blk", None, None),
            P("section", None),
            P("section", None, None),
            P("section", None, None),
        ),
        out_specs=P("blk", "section"),
        check_vma=False,
    )
```

```python
import functools
import math

import jax
import jax.numpy as jnp
from jax import lax
from jax.experimental import pallas as pl
from jax.experimental.pallas import tpu as pltpu
from jax.sharding import PartitionSpec as P

BLOCK = 64
MICRO = 8
PARTS = 2
CHUNKS = MICRO * PARTS
LAG_A = 1
LAG_U = 2
EPSILON = 1e-05
NEGATIVE = -1e30
TAIL = 128
MESH = pl.DeviceIdType.MESH
F32 = jnp.float32
BF16 = jnp.bfloat16


def kernel(
    shards,
    layers,
    hidden,
    gain,
    wq_hbm,
    wo_hbm,
    cache_hbm,
    exit_rows,
    length_rows,
    out,
    wq,
    wo,
    cache,
    inb,
    outb,
    exits,
    lens,
    accs,
    rs_send,
    rs_recv,
    att,
    w_sem,
    hid_ss,
    in_rs,
    rs_ss,
    rs_rs,
    ag_ss,
    ag_rs,
    st_ss,
    out_rs,
):
    me = lax.axis_index("section")
    y = me // shards
    x = me % shards
    last = layers - 1
    group, span = inb.shape[3:]
    rows = shards * group
    query_width = wo.shape[1]
    width = wq.shape[2]
    head = (width - query_width) // 2
    heads = query_width // head
    context = cache.shape[0] // (CHUNKS * group)
    total_width = span * shards * layers

    def remote(src, dst, send_sem, recv_sem, target):
        return pltpu.make_async_remote_copy(
            src_ref=src,
            dst_ref=dst,
            send_sem=send_sem,
            recv_sem=recv_sem,
            device_id={"section": target},
            device_id_type=MESH,
        )

    def row_peer(d):
        return y * shards + (x + d) % shards

    wq_copies = [
        pltpu.make_async_copy(wq_hbm.at[pl.ds(j * span, span)], wq.at[j], w_sem.at[j])
        for j in range(layers)
    ]
    wo_copies = [
        pltpu.make_async_copy(
            wo_hbm.at[:, pl.ds(j * span, span)], wo.at[j], w_sem.at[layers + j]
        )
        for j in range(layers)
    ]
    cache_copy = pltpu.make_async_copy(cache_hbm, cache, w_sem.at[2 * layers])
    for copy in wq_copies:
        copy.start()
    cache_copy.start()
    for copy in wo_copies:
        copy.start()

    barrier = pltpu.get_barrier_semaphore()
    for d in range(1, shards):
        pl.semaphore_signal(
            barrier, inc=1, device_id={"section": row_peer(d)}, device_id_type=MESH
        )
    for d in range(1, layers):
        pl.semaphore_signal(
            barrier,
            inc=1,
            device_id={"section": ((y + d) % layers) * shards + x},
            device_id_type=MESH,
        )
    pl.semaphore_wait(barrier, shards + layers - 2)

    rounds = MICRO // layers
    place = (layers - y) % layers

    pieces = [
        (q, h, j) for q in range(rounds) for h in range(PARTS) for j in range(layers)
    ]

    def hidden_piece(q, h, j):
        return hidden.at[q, :, h, :, pl.ds(j * span, span)]

    def hidden_copy(q, h, j):
        i = (q * layers + place) * PARTS + h
        return remote(
            hidden_piece(q, h, j), inb.at[i, j], hid_ss.at[q, h, j], in_rs.at[i, j], x
        )

    @pl.when(y == 0)
    def _():
        for q, h, j in pieces:
            i = q * layers * PARTS + h
            pltpu.make_async_copy(
                hidden_piece(q, h, j), inb.at[i, j], in_rs.at[i, j]
            ).start()

    @pl.when(y != 0)
    def _():
        for q, h, j in pieces:
            hidden_copy(q, h, j).start()

    for r in range(exit_rows.shape[0]):
        for source, target in ((exit_rows, exits), (length_rows, lens)):
            spread = jnp.broadcast_to(source[r : r + 1, :], (TAIL, TAIL)).T
            count = TAIL // BLOCK
            target[r * count : (r + 1) * count] = spread.reshape(
                (count,) + target.shape[1:]
            )

    def rs_copy(i, d):
        target = (x + d) % shards
        return remote(
            rs_send.at[i, target],
            rs_recv.at[i, x],
            rs_ss.at[i, d - 1],
            rs_rs.at[i, x],
            row_peer(d),
        )

    def rs_arrival(i, d):
        source = (x + d) % shards
        return remote(
            rs_send.at[i, source],
            rs_recv.at[i, source],
            rs_ss.at[i, d - 1],
            rs_rs.at[i, source],
            row_peer(d),
        )

    def ag_copy(i, d):
        return remote(
            att.at[i, x], att.at[i, x], ag_ss.at[i, d - 1], ag_rs.at[i, x], row_peer(d)
        )

    def ag_arrival(i, d):
        source = (x + d) % shards
        return remote(
            att.at[i, source],
            att.at[i, source],
            ag_ss.at[i, d - 1],
            ag_rs.at[i, source],
            row_peer(d),
        )

    def state_copy(i, j):
        return remote(
            outb.at[i, j],
            inb.at[i, j],
            st_ss.at[i, j],
            in_rs.at[i, j],
            (me + shards) % (shards * layers),
        )

    def tokens(ref, i):
        return ref.at[i // PARTS, :, i % PARTS]

    def result_copy(i, j):
        return remote(
            outb.at[i, j], tokens(out, i), st_ss.at[i, j], out_rs.at[i], j * shards + x
        )

    def project(i):
        squares = jnp.zeros((rows, TAIL), F32)
        acc = None
        for j in range(layers):

            @pl.when(i == 0)
            def _():
                wq_copies[j].wait()

            state_copy(i, j).wait_recv()
            state = inb[i, j].astype(F32).reshape(rows, span)
            scaled = (state * gain[:, pl.ds(j * span, span)].astype(F32)).astype(BF16)
            squared = state * state
            for n in range(span // TAIL):
                squares = squares + squared[:, n * TAIL : (n + 1) * TAIL]
            part = jnp.dot(scaled, wq[j], preferred_element_type=F32)
            acc = part if acc is None else acc + part
        total = jnp.sum(squares, axis=1, keepdims=True)
        coarse = total.astype(BF16).astype(F32)
        lane = lax.broadcasted_iota(jnp.int32, (rows, TAIL), 1)
        tail = jnp.where(lane < TAIL // 2, coarse, total - coarse)
        for g in range(shards):
            part = slice(g * group, (g + 1) * group)
            accs[i, g, :, :width] = acc[part]
            accs[i, g, :, width:] = tail[part]
            rs_send[i, g, :, :width] = acc[part].astype(BF16)
            rs_send[i, g, :, width:] = tail[part].astype(BF16)
        for d in (2, 1, 3):
            rs_copy(i, d).start()

    def attend(i):
        @pl.when(i == 0)
        def _():
            cache_copy.wait()

        summed = accs[i, x]
        for d in (1, 3, 2):
            rs_arrival(i, d).wait_recv()
        for d in (1, 3, 2):
            summed = summed + rs_recv[i, (x + d) % shards].astype(F32)
        squares = jnp.sum(summed[:, width:], axis=1, keepdims=True) * (2.0 / TAIL)
        scale = lax.rsqrt(squares / total_width + EPSILON)
        fitted = summed[:, :width] * scale
        query = fitted[:, :query_width] * (1.0 / math.sqrt(head))
        query = jnp.concatenate(
            [query[:, h * head : (h + 1) * head] for h in range(heads)], axis=0
        ).astype(BF16)
        key_new = fitted[:, query_width : query_width + head].astype(BF16).astype(F32)
        value_new = fitted[:, query_width + head :].astype(BF16).astype(F32)
        key_new = jnp.concatenate([key_new] * heads, axis=0)
        value_new = jnp.concatenate([value_new] * heads, axis=0)
        held = group * context
        keys = cache[pl.ds(pl.multiple_of(i * held, held), held), :head]
        values = cache[pl.ds(pl.multiple_of(i * held, held), held), head:]
        scores = lax.dot_general(
            query, keys, (((1,), (1,)), ((), ())), preferred_element_type=F32
        )
        own = jnp.sum(query.astype(F32) * key_new, axis=1, keepdims=True)
        reach = lens[i // PARTS, x, i % PARTS]
        reach = jnp.concatenate([reach] * (held // TAIL), axis=1)
        reach = jnp.concatenate([reach] * heads, axis=0)
        shape = (heads * group, held)
        row = lax.broadcasted_iota(jnp.int32, shape, 0)
        column = lax.broadcasted_iota(jnp.int32, shape, 1)
        offset = column - (row % group) * context
        usable = (offset >= 0) & (offset < reach)
        scores = jnp.where(usable, scores, NEGATIVE)
        top = jnp.maximum(jnp.max(scores, axis=1, keepdims=True), own)
        raw = jnp.where(usable, jnp.exp(scores - top), 0.0)
        raw_own = jnp.exp(own - top)
        total = jnp.sum(raw, axis=1, keepdims=True) + raw_own
        inverse = 1.0 / total
        weights = (raw * inverse).astype(BF16)
        own_weight = (raw_own * inverse).astype(BF16).astype(F32)
        attended = jnp.dot(weights, values, preferred_element_type=F32)
        attended = attended + own_weight * value_new
        att[i, x] = jnp.concatenate(
            [attended[h * group : (h + 1) * group] for h in range(heads)], axis=1
        ).astype(BF16)
        for d in (2, 1, 3):
            ag_copy(i, d).start()

    def update(i):
        for d in (1, 3, 2):
            ag_arrival(i, d).wait_recv()
        attended = att[i].astype(F32).reshape(rows, query_width).astype(BF16)
        depth = exits[i // PARTS, :, i % PARTS].reshape(rows, TAIL)
        active = jnp.concatenate([depth] * (span // TAIL), axis=1) > y
        for j in range(layers):

            @pl.when(i == 0)
            def _():
                wo_copies[j].wait()

            state = inb[i, j].astype(F32).reshape(rows, span)
            branch = jnp.dot(attended, wo[j], preferred_element_type=F32)
            updated = jnp.where(active, state + branch, state)
            updated = updated.reshape(shards, group, span).astype(BF16)
            outb[i, j] = updated

            @pl.when(y < last)
            def _():
                state_copy(i, j).start()

            if j < last:

                @pl.when(y == last)
                def _():
                    result_copy(i, j).start()

            else:

                @pl.when(y == last)
                def _():
                    out[i // PARTS, :, i % PARTS] = updated

    def step(i, carry):
        @pl.when(i < CHUNKS)
        def _():
            project(i)

        @pl.when((i >= LAG_A) & (i < CHUNKS + LAG_A))
        def _():
            attend(i - LAG_A)

        @pl.when(i >= LAG_U)
        def _():
            update(i - LAG_U)

        return carry

    lax.fori_loop(0, CHUNKS + LAG_U, step, 0)

    def finish(i, carry):
        for d in range(1, shards):
            rs_copy(i, d).wait_send()
            ag_copy(i, d).wait_send()
        for j in range(layers):

            @pl.when(y < last)
            def _():
                state_copy(i, j).wait_send()

            if j < last:

                @pl.when(y == last)
                def _():
                    result_copy(i, j).wait_send()

        @pl.when(y < last)
        def _():
            result_copy(i, 0).wait_recv()

        return carry

    lax.fori_loop(0, CHUNKS, finish, 0)

    @pl.when(y != 0)
    def _():
        for q, h, j in pieces:
            hidden_copy(q, h, j).wait_send()


def body(hidden, exit_layer, lengths, kv_cache, norm_gain, w_qkv, w_out):
    devices = lax.axis_size("section")
    shards = max(2, devices // 4)
    layers = devices // shards
    own_hidden = hidden[0]
    proj_weight = w_qkv[0]
    out_weight = w_out[0]
    tokens = exit_layer.shape[0]
    quarter, width = proj_weight.shape
    query_width = out_weight.shape[0]
    span = quarter // layers
    group = BLOCK // shards // PARTS
    cache_rows = kv_cache.shape[1] * kv_cache.shape[2]
    cache = kv_cache.reshape(cache_rows, kv_cache.shape[3])
    exits = exit_layer.reshape(tokens // TAIL, TAIL)
    lens = lengths.reshape(tokens // TAIL, TAIL)
    own_hidden = own_hidden.reshape(MICRO // layers, shards, PARTS, group, quarter)
    anywhere = pl.BlockSpec(memory_space=pl.ANY)
    vmem = pl.BlockSpec(memory_space=pltpu.VMEM)
    dma = pltpu.SemaphoreType.DMA
    column = (MICRO, shards, PARTS, group, TAIL)
    settled = pl.pallas_call(
        functools.partial(kernel, shards, layers),
        out_shape=jax.ShapeDtypeStruct((MICRO, shards, PARTS, group, span), BF16),
        in_specs=[anywhere, vmem, anywhere, anywhere, anywhere, vmem, vmem],
        out_specs=vmem,
        scratch_shapes=[
            pltpu.VMEM((layers, span, width), BF16),
            pltpu.VMEM((layers, query_width, span), BF16),
            pltpu.VMEM(cache.shape, BF16),
            pltpu.VMEM((CHUNKS, layers, shards, group, span), BF16),
            pltpu.VMEM((CHUNKS, layers, shards, group, span), BF16),
            pltpu.VMEM(column, jnp.int32),
            pltpu.VMEM(column, jnp.int32),
            pltpu.VMEM((CHUNKS, shards, group, width + TAIL), F32),
            pltpu.VMEM((CHUNKS, shards, group, width + TAIL), BF16),
            pltpu.VMEM((CHUNKS, shards, group, width + TAIL), BF16),
            pltpu.VMEM((CHUNKS, shards, group, query_width), BF16),
            dma((2 * layers + 1,)),
            dma((MICRO // layers, PARTS, layers)),
            dma((CHUNKS, layers)),
            dma((CHUNKS, shards - 1)),
            dma((CHUNKS, shards)),
            dma((CHUNKS, shards - 1)),
            dma((CHUNKS, shards)),
            dma((CHUNKS, layers)),
            dma((CHUNKS,)),
        ],
        compiler_params=pltpu.CompilerParams(
            collective_id=0, has_side_effects=True, vmem_limit_bytes=56 << 20
        ),
    )(own_hidden, norm_gain, proj_weight, out_weight, cache, exits, lens)
    return settled.reshape(tokens, span)


def solution(mesh):
    return jax.shard_map(
        body,
        mesh=mesh,
        in_specs=(
            P("section", "blk", None),
            P("blk"),
            P("blk"),
            P("section", "blk", None, None),
            P("section", None),
            P("section", None, None),
            P("section", None, None),
        ),
        out_specs=P("blk", "section"),
        check_vma=False,
    )
```

```python
import functools
import math

import jax
import jax.numpy as jnp
from jax import lax
from jax.experimental import pallas as pl
from jax.experimental.pallas import tpu as pltpu
from jax.sharding import PartitionSpec as P

BLOCK = 64
MICRO = 8
PARTS = 2
CHUNKS = MICRO * PARTS
CONTEXT = 16
SORTED = 4
KEEP = 16
MAIN = 8
DEEP = MAIN + 1
TOTAL = DEEP + MAIN
POSITION = ((0, 1, 9, 10), (2, 4, 11, 13), (6, 7, 15, 16), (3, 5, 12, 14))
LAG_A = 1
LAG_U = 2
EPSILON = 1e-05
NEGATIVE = -1e30
TAIL = 128
MESH = pl.DeviceIdType.MESH
F32 = jnp.float32
BF16 = jnp.bfloat16


def full_kernel(
    shards,
    layers,
    hidden,
    gain,
    wq_hbm,
    wo_hbm,
    cache_hbm,
    exit_rows,
    length_rows,
    out,
    wq,
    wo,
    cache,
    inb,
    outb,
    exits,
    lens,
    accs,
    rs_send,
    rs_recv,
    att,
    w_sem,
    hid_ss,
    in_rs,
    rs_ss,
    rs_rs,
    ag_ss,
    ag_rs,
    st_ss,
    out_rs,
):
    me = lax.axis_index("section")
    y = me // shards
    x = me % shards
    last = layers - 1
    group, span = inb.shape[3:]
    rows = shards * group
    query_width = wo.shape[1]
    width = wq.shape[2]
    head = (width - query_width) // 2
    heads = query_width // head
    context = cache.shape[0] // (CHUNKS * group)
    total_width = span * shards * layers

    def remote(src, dst, send_sem, recv_sem, target):
        return pltpu.make_async_remote_copy(
            src_ref=src,
            dst_ref=dst,
            send_sem=send_sem,
            recv_sem=recv_sem,
            device_id={"section": target},
            device_id_type=MESH,
        )

    def row_peer(d):
        return y * shards + (x + d) % shards

    wq_copies = [
        pltpu.make_async_copy(wq_hbm.at[pl.ds(j * span, span)], wq.at[j], w_sem.at[j])
        for j in range(layers)
    ]
    wo_copies = [
        pltpu.make_async_copy(
            wo_hbm.at[:, pl.ds(j * span, span)], wo.at[j], w_sem.at[layers + j]
        )
        for j in range(layers)
    ]
    cache_copy = pltpu.make_async_copy(cache_hbm, cache, w_sem.at[2 * layers])
    for copy in wq_copies:
        copy.start()
    cache_copy.start()
    for copy in wo_copies:
        copy.start()

    barrier = pltpu.get_barrier_semaphore()
    for d in range(1, shards):
        pl.semaphore_signal(
            barrier, inc=1, device_id={"section": row_peer(d)}, device_id_type=MESH
        )
    for d in range(1, layers):
        pl.semaphore_signal(
            barrier,
            inc=1,
            device_id={"section": ((y + d) % layers) * shards + x},
            device_id_type=MESH,
        )
    pl.semaphore_wait(barrier, shards + layers - 2)

    rounds = MICRO // layers
    place = (layers - y) % layers

    pieces = [
        (q, h, j) for q in range(rounds) for h in range(PARTS) for j in range(layers)
    ]

    def hidden_piece(q, h, j):
        return hidden.at[q, :, h, :, pl.ds(j * span, span)]

    def hidden_copy(q, h, j):
        i = (q * layers + place) * PARTS + h
        return remote(
            hidden_piece(q, h, j), inb.at[i, j], hid_ss.at[q, h, j], in_rs.at[i, j], x
        )

    @pl.when(y == 0)
    def _():
        for q, h, j in pieces:
            i = q * layers * PARTS + h
            pltpu.make_async_copy(
                hidden_piece(q, h, j), inb.at[i, j], in_rs.at[i, j]
            ).start()

    @pl.when(y != 0)
    def _():
        for q, h, j in pieces:
            hidden_copy(q, h, j).start()

    for r in range(exit_rows.shape[0]):
        for source, target in ((exit_rows, exits), (length_rows, lens)):
            spread = jnp.broadcast_to(source[r : r + 1, :], (TAIL, TAIL)).T
            count = TAIL // BLOCK
            target[r * count : (r + 1) * count] = spread.reshape(
                (count,) + target.shape[1:]
            )

    def rs_copy(i, d):
        target = (x + d) % shards
        return remote(
            rs_send.at[i, target],
            rs_recv.at[i, x],
            rs_ss.at[i, d - 1],
            rs_rs.at[i, x],
            row_peer(d),
        )

    def rs_arrival(i, d):
        source = (x + d) % shards
        return remote(
            rs_send.at[i, source],
            rs_recv.at[i, source],
            rs_ss.at[i, d - 1],
            rs_rs.at[i, source],
            row_peer(d),
        )

    def ag_copy(i, d):
        return remote(
            att.at[i, x], att.at[i, x], ag_ss.at[i, d - 1], ag_rs.at[i, x], row_peer(d)
        )

    def ag_arrival(i, d):
        source = (x + d) % shards
        return remote(
            att.at[i, source],
            att.at[i, source],
            ag_ss.at[i, d - 1],
            ag_rs.at[i, source],
            row_peer(d),
        )

    def state_copy(i, j):
        return remote(
            outb.at[i, j],
            inb.at[i, j],
            st_ss.at[i, j],
            in_rs.at[i, j],
            (me + shards) % (shards * layers),
        )

    def tokens(ref, i):
        return ref.at[i // PARTS, :, i % PARTS]

    def result_copy(i, j):
        return remote(
            outb.at[i, j], tokens(out, i), st_ss.at[i, j], out_rs.at[i], j * shards + x
        )

    def project(i):
        squares = jnp.zeros((rows, TAIL), F32)
        acc = None
        for j in range(layers):

            @pl.when(i == 0)
            def _():
                wq_copies[j].wait()

            state_copy(i, j).wait_recv()
            state = inb[i, j].astype(F32).reshape(rows, span)
            scaled = (state * gain[:, pl.ds(j * span, span)].astype(F32)).astype(BF16)
            squared = state * state
            for n in range(span // TAIL):
                squares = squares + squared[:, n * TAIL : (n + 1) * TAIL]
            part = jnp.dot(scaled, wq[j], preferred_element_type=F32)
            acc = part if acc is None else acc + part
        total = jnp.sum(squares, axis=1, keepdims=True)
        coarse = total.astype(BF16).astype(F32)
        lane = lax.broadcasted_iota(jnp.int32, (rows, TAIL), 1)
        tail = jnp.where(lane < TAIL // 2, coarse, total - coarse)
        for g in range(shards):
            part = slice(g * group, (g + 1) * group)
            accs[i, g, :, :width] = acc[part]
            accs[i, g, :, width:] = tail[part]
            rs_send[i, g, :, :width] = acc[part].astype(BF16)
            rs_send[i, g, :, width:] = tail[part].astype(BF16)
        for d in (2, 1, 3):
            rs_copy(i, d).start()

    def attend(i):
        @pl.when(i == 0)
        def _():
            cache_copy.wait()

        summed = accs[i, x]
        for d in (1, 3, 2):
            rs_arrival(i, d).wait_recv()
        for d in (1, 3, 2):
            summed = summed + rs_recv[i, (x + d) % shards].astype(F32)
        squares = jnp.sum(summed[:, width:], axis=1, keepdims=True) * (2.0 / TAIL)
        scale = lax.rsqrt(squares / total_width + EPSILON)
        fitted = summed[:, :width] * scale
        query = fitted[:, :query_width] * (1.0 / math.sqrt(head))
        query = jnp.concatenate(
            [query[:, h * head : (h + 1) * head] for h in range(heads)], axis=0
        ).astype(BF16)
        key_new = fitted[:, query_width : query_width + head].astype(BF16).astype(F32)
        value_new = fitted[:, query_width + head :].astype(BF16).astype(F32)
        key_new = jnp.concatenate([key_new] * heads, axis=0)
        value_new = jnp.concatenate([value_new] * heads, axis=0)
        held = group * context
        keys = cache[pl.ds(pl.multiple_of(i * held, held), held), :head]
        values = cache[pl.ds(pl.multiple_of(i * held, held), held), head:]
        scores = lax.dot_general(
            query, keys, (((1,), (1,)), ((), ())), preferred_element_type=F32
        )
        own = jnp.sum(query.astype(F32) * key_new, axis=1, keepdims=True)
        reach = lens[i // PARTS, x, i % PARTS]
        reach = jnp.concatenate([reach] * (held // TAIL), axis=1)
        reach = jnp.concatenate([reach] * heads, axis=0)
        shape = (heads * group, held)
        row = lax.broadcasted_iota(jnp.int32, shape, 0)
        column = lax.broadcasted_iota(jnp.int32, shape, 1)
        offset = column - (row % group) * context
        usable = (offset >= 0) & (offset < reach)
        scores = jnp.where(usable, scores, NEGATIVE)
        top = jnp.maximum(jnp.max(scores, axis=1, keepdims=True), own)
        raw = jnp.where(usable, jnp.exp(scores - top), 0.0)
        raw_own = jnp.exp(own - top)
        total = jnp.sum(raw, axis=1, keepdims=True) + raw_own
        inverse = 1.0 / total
        weights = (raw * inverse).astype(BF16)
        own_weight = (raw_own * inverse).astype(BF16).astype(F32)
        attended = jnp.dot(weights, values, preferred_element_type=F32)
        attended = attended + own_weight * value_new
        att[i, x] = jnp.concatenate(
            [attended[h * group : (h + 1) * group] for h in range(heads)], axis=1
        ).astype(BF16)
        for d in (2, 1, 3):
            ag_copy(i, d).start()

    def update(i):
        for d in (1, 3, 2):
            ag_arrival(i, d).wait_recv()
        attended = att[i].astype(F32).reshape(rows, query_width).astype(BF16)
        depth = exits[i // PARTS, :, i % PARTS].reshape(rows, TAIL)
        active = jnp.concatenate([depth] * (span // TAIL), axis=1) > y
        for j in range(layers):

            @pl.when(i == 0)
            def _():
                wo_copies[j].wait()

            state = inb[i, j].astype(F32).reshape(rows, span)
            branch = jnp.dot(attended, wo[j], preferred_element_type=F32)
            updated = jnp.where(active, state + branch, state)
            updated = updated.reshape(shards, group, span).astype(BF16)
            outb[i, j] = updated

            @pl.when(y < last)
            def _():
                state_copy(i, j).start()

            if j < last:

                @pl.when(y == last)
                def _():
                    result_copy(i, j).start()

            else:

                @pl.when(y == last)
                def _():
                    out[i // PARTS, :, i % PARTS] = updated

    def step(i, carry):
        @pl.when(i < CHUNKS)
        def _():
            project(i)

        @pl.when((i >= LAG_A) & (i < CHUNKS + LAG_A))
        def _():
            attend(i - LAG_A)

        @pl.when(i >= LAG_U)
        def _():
            update(i - LAG_U)

        return carry

    lax.fori_loop(0, CHUNKS + LAG_U, step, 0)

    def finish(i, carry):
        for d in range(1, shards):
            rs_copy(i, d).wait_send()
            ag_copy(i, d).wait_send()
        for j in range(layers):

            @pl.when(y < last)
            def _():
                state_copy(i, j).wait_send()

            if j < last:

                @pl.when(y == last)
                def _():
                    result_copy(i, j).wait_send()

        @pl.when(y < last)
        def _():
            result_copy(i, 0).wait_recv()

        return carry

    lax.fori_loop(0, CHUNKS, finish, 0)

    @pl.when(y != 0)
    def _():
        for q, h, j in pieces:
            hidden_copy(q, h, j).wait_send()


def early_kernel(
    shards,
    layers,
    hidden,
    gain,
    wq_hbm,
    wo_hbm,
    cache_hbm,
    exit_rows,
    length_rows,
    out,
    wq,
    wo,
    cache,
    inb,
    outb,
    hid,
    staged,
    own_pick,
    late_pick,
    target,
    settled,
    exits,
    lens,
    starts,
    accs,
    rs_send,
    rs_recv,
    att,
    w_sem,
    hid_in,
    hid_ss,
    turn,
    in_rs,
    rs_ss,
    rs_rs,
    ag_ss,
    ag_rs,
    st_ss,
    out_rs,
):
    me = lax.axis_index("section")
    y = me // shards
    x = me % shards
    last = layers - 1
    group, span = inb.shape[3:]
    rows = shards * group
    query_width = wo.shape[1]
    width = wq.shape[2]
    head = (width - query_width) // 2
    heads = query_width // head
    context = CONTEXT
    count = DEEP + MAIN * ((last - y) // last)
    total_width = span * shards * layers

    def remote(src, dst, send_sem, recv_sem, target):
        return pltpu.make_async_remote_copy(
            src_ref=src,
            dst_ref=dst,
            send_sem=send_sem,
            recv_sem=recv_sem,
            device_id={"section": target},
            device_id_type=MESH,
        )

    def row_peer(d):
        return y * shards + (x + d) % shards

    wq_copies = [
        pltpu.make_async_copy(wq_hbm.at[pl.ds(j * span, span)], wq.at[j], w_sem.at[j])
        for j in range(layers)
    ]
    wo_copies = [
        pltpu.make_async_copy(
            wo_hbm.at[:, pl.ds(j * span, span)], wo.at[j], w_sem.at[layers + j]
        )
        for j in range(layers)
    ]
    cache_copy = pltpu.make_async_copy(cache_hbm, cache, w_sem.at[2 * layers])
    hid_copy = pltpu.make_async_copy(hidden, hid, hid_in.at[0])
    hid_copy.start()
    for copy in wq_copies:
        copy.start()
    cache_copy.start()
    for copy in wo_copies:
        copy.start()

    barrier = pltpu.get_barrier_semaphore()
    for d in range(1, shards):
        pl.semaphore_signal(
            barrier, inc=1, device_id={"section": row_peer(d)}, device_id_type=MESH
        )
    for d in range(1, layers):
        pl.semaphore_signal(
            barrier,
            inc=1,
            device_id={"section": ((y + d) % layers) * shards + x},
            device_id_type=MESH,
        )

    wide = (TAIL, TAIL)
    t0 = lax.broadcasted_iota(jnp.int32, wide, 0)
    t1 = lax.broadcasted_iota(jnp.int32, wide, 1)
    g0 = (t0 & (BLOCK - 1)) >> 4
    g1 = (t1 & (BLOCK - 1)) >> 4
    same = g0 == g1
    lane_group = (t1 & 31) >> 3
    lane_rank = ((t1 >> 5) << 3) + (t1 & 7)
    slot_row = lax.broadcasted_iota(jnp.int32, (rows, TAIL), 0)
    low_half = t1 < BLOCK
    base_lane = jnp.zeros((1, TAIL), jnp.int32)
    base_column = jnp.zeros((TAIL, 1), jnp.int32)
    late = jnp.zeros((rows, 3 * TAIL), F32)

    def piece_row(ref, p):
        first = jnp.broadcast_to(ref[p // 2 : p // 2 + 1, :], wide)
        second = jnp.broadcast_to(ref[p // 2 + 2 : p // 2 + 3, :], wide)
        if p % 2 == 0:
            return jnp.where(low_half, first, pltpu.roll(second, BLOCK, 1))
        return jnp.where(low_half, pltpu.roll(first, BLOCK, 1), second)

    def number(mask):
        return jnp.where(mask, 1.0, 0.0)

    for p in range(layers):
        exit_row = piece_row(exit_rows, p)
        exit_column = exit_row.T
        length_column = piece_row(length_rows, p).T
        ahead = same & (
            (exit_column > exit_row) | ((exit_column == exit_row) & (t0 < t1))
        )
        rank_lane = jnp.sum(number(ahead), axis=0, keepdims=True).astype(jnp.int32)
        behind = same & (
            (exit_row > exit_column) | ((exit_row == exit_column) & (t1 < t0))
        )
        rank_column = jnp.sum(number(behind), axis=1, keepdims=True).astype(jnp.int32)
        deep_column = jnp.sum(
            number(same & (exit_row > 1)), axis=1, keepdims=True
        ).astype(jnp.int32)
        deep_lane = jnp.sum(
            number((exit_column > 1) & (g0 == lane_group)), axis=0, keepdims=True
        ).astype(jnp.int32)
        order_lane = ((rank_lane >> 3) << 5) + (g1 << 3) + (rank_lane & 7)
        order_column = ((rank_column >> 3) << 5) + (g0 << 3) + (rank_column & 7)
        pick = number(order_lane == t0).astype(BF16)

        @pl.when(y == (layers - p) % layers)
        def _():
            own_pick[...] = pick

        natural = ((p + layers * (t0 >> 6)) << 4) + (t0 & 15)
        facts = jnp.concatenate([exit_column, length_column, natural], axis=1)
        sorted_facts = jnp.dot(
            pick, facts.astype(F32).astype(BF16), preferred_element_type=F32
        )
        for c in range(SORTED):
            block = sorted_facts[c * rows : (c + 1) * rows].astype(jnp.int32)
            block = block.reshape(shards, group, 3 * TAIL)
            exits[POSITION[p][c]] = block[:, :, :TAIL]
            lens[POSITION[p][c]] = block[:, :, TAIL : 2 * TAIL]
            starts[POSITION[p][c]] = block[:, :, 2 * TAIL :] * context
        chosen = (
            (lane_rank[:rows] >= KEEP)
            & (lane_rank[:rows] < deep_lane)
            & (lane_group[:rows] == (slot_row >> 3))
            & (base_lane + lane_rank[:rows] - KEEP == (slot_row & 7))
        )
        chosen = number(chosen).astype(BF16)
        late_pick[p] = chosen
        late = late + jnp.dot(
            chosen, sorted_facts.astype(BF16), preferred_element_type=F32
        )
        moved = (rank_column >= KEEP) & (rank_column < deep_column)
        target[p] = jnp.where(
            moved,
            TAIL + (g0 << 3) + base_column + rank_column - KEEP,
            order_column,
        )
        base_lane = base_lane + jnp.maximum(deep_lane - KEEP, 0)
        base_column = base_column + jnp.maximum(deep_column - KEEP, 0)
    late = late.astype(jnp.int32).reshape(shards, group, 3 * TAIL)
    exits[MAIN] = late[:, :, :TAIL]
    lens[MAIN] = late[:, :, TAIL : 2 * TAIL]
    starts[MAIN] = late[:, :, 2 * TAIL :] * context

    hid_copy.wait()
    for j in range(layers):
        ordered = jnp.dot(
            own_pick[...],
            hid[:, j * span : (j + 1) * span],
            preferred_element_type=F32,
        )
        ordered = ordered.reshape(SORTED, shards, group, span).astype(BF16)

        @pl.when(y == 0)
        def _():
            for c in range(SORTED):
                inb[POSITION[0][c], j] = ordered[c]

        @pl.when(y != 0)
        def _():
            for c in range(SORTED):
                staged[c, j] = ordered[c]

    pl.semaphore_wait(barrier, shards + layers - 2)

    def hidden_copy(p, c, j):
        i = POSITION[p][c]
        return remote(
            staged.at[c, j], inb.at[i, j], hid_ss.at[c, j], in_rs.at[i, j], x
        )

    def hidden_start(p, chunks):
        for c in chunks:
            for j in range(layers):
                hidden_copy(p, c, j).start()

    def hidden_sent(p, chunks):
        for c in chunks:
            for j in range(layers):
                hidden_copy(p, c, j).wait_send()

    for p in (1, 3):

        @pl.when(y == layers - p)
        def _():
            hidden_start(p, (0, 1))
            hidden_sent(p, (0, 1))
            pl.semaphore_signal(
                turn, inc=1, device_id={"section": 2 * shards + x}, device_id_type=MESH
            )
            hidden_start(p, (2, 3))

    @pl.when(y == 2)
    def _():
        pl.semaphore_wait(turn, 2)
        hidden_start(2, (0, 1, 2, 3))

    def rs_copy(i, d):
        target = (x + d) % shards
        return remote(
            rs_send.at[i, target],
            rs_recv.at[i, x],
            rs_ss.at[i, d - 1],
            rs_rs.at[i, x],
            row_peer(d),
        )

    def rs_arrival(i, d):
        source = (x + d) % shards
        return remote(
            rs_send.at[i, source],
            rs_recv.at[i, source],
            rs_ss.at[i, d - 1],
            rs_rs.at[i, source],
            row_peer(d),
        )

    def ag_copy(i, d):
        return remote(
            att.at[i, x], att.at[i, x], ag_ss.at[i, d - 1], ag_rs.at[i, x], row_peer(d)
        )

    def ag_arrival(i, d):
        source = (x + d) % shards
        return remote(
            att.at[i, source],
            att.at[i, source],
            ag_ss.at[i, d - 1],
            ag_rs.at[i, source],
            row_peer(d),
        )

    def state_copy(i, j):
        return remote(
            outb.at[i, j],
            inb.at[i, j],
            st_ss.at[i, j],
            in_rs.at[i, j],
            (me + shards) % (shards * layers),
        )

    def result_copy(i, j):
        return remote(
            outb.at[i, j], settled.at[i], st_ss.at[i, j], out_rs.at[i], j * shards + x
        )

    def gather_late():
        for c in range(2, SORTED):
            for p in range(1, layers):
                for j in range(layers):
                    state_copy(POSITION[p][c], j).wait_recv()
        for j in range(layers):
            found = None
            for p in range(layers):
                held = [inb[POSITION[p][c], j].astype(F32) for c in range(2, SORTED)]
                held = [jnp.zeros_like(part) for part in held] + held
                held = jnp.concatenate([part.reshape(rows, span) for part in held], axis=0)
                part = jnp.dot(
                    late_pick[p], held.astype(BF16), preferred_element_type=F32
                )
                found = part if found is None else found + part
            inb[MAIN, j] = found.reshape(shards, group, span).astype(BF16)

    def project(i):
        squares = jnp.zeros((rows, TAIL), F32)
        acc = None
        for j in range(layers):

            @pl.when(i == 0)
            def _():
                wq_copies[j].wait()

            @pl.when((y > 0) | ((i > 1) & (i < MAIN)))
            def _():
                state_copy(i, j).wait_recv()

            state = inb[i, j].astype(F32).reshape(rows, span)
            scaled = (state * gain[:, pl.ds(j * span, span)].astype(F32)).astype(BF16)
            squared = state * state
            for n in range(span // TAIL):
                squares = squares + squared[:, n * TAIL : (n + 1) * TAIL]
            part = jnp.dot(scaled, wq[j], preferred_element_type=F32)
            acc = part if acc is None else acc + part
        total = jnp.sum(squares, axis=1, keepdims=True)
        coarse = total.astype(BF16).astype(F32)
        lane = lax.broadcasted_iota(jnp.int32, (rows, TAIL), 1)
        tail = jnp.where(lane < TAIL // 2, coarse, total - coarse)
        for g in range(shards):
            part = slice(g * group, (g + 1) * group)
            accs[i, g, :, :width] = acc[part]
            accs[i, g, :, width:] = tail[part]
            rs_send[i, g, :, :width] = acc[part].astype(BF16)
            rs_send[i, g, :, width:] = tail[part].astype(BF16)
        for d in (2, 1, 3):
            rs_copy(i, d).start()

    def attend(i):
        @pl.when(i == 0)
        def _():
            cache_copy.wait()

        b = i - DEEP * (i // DEEP)
        p = ((b + 6) // 8) * (1 - b // 6) * (1 + 2 * (b % 2)) + 2 * (b // 6)
        half = shards * shards * context

        @pl.when(i == MAIN)
        def _():
            attend_over(i, [(0, cache.shape[0])])

        @pl.when(i != MAIN)
        def _():
            attend_over(
                i,
                [
                    (pl.multiple_of(p * half, half), half),
                    (pl.multiple_of((p + layers) * half, half), half),
                ],
            )

    def attend_over(i, pieces):

        summed = accs[i, x]
        for d in (1, 3, 2):
            rs_arrival(i, d).wait_recv()
        for d in (1, 3, 2):
            summed = summed + rs_recv[i, (x + d) % shards].astype(F32)
        squares = jnp.sum(summed[:, width:], axis=1, keepdims=True) * (2.0 / TAIL)
        scale = lax.rsqrt(squares / total_width + EPSILON)
        fitted = summed[:, :width] * scale
        query = fitted[:, :query_width] * (1.0 / math.sqrt(head))
        query = jnp.concatenate(
            [query[:, h * head : (h + 1) * head] for h in range(heads)], axis=0
        ).astype(BF16)
        key_new = fitted[:, query_width : query_width + head].astype(BF16).astype(F32)
        value_new = fitted[:, query_width + head :].astype(BF16).astype(F32)
        key_new = jnp.concatenate([key_new] * heads, axis=0)
        value_new = jnp.concatenate([value_new] * heads, axis=0)
        keys = jnp.concatenate(
            [cache[pl.ds(at, size), :head] for at, size in pieces], axis=0
        )
        values = jnp.concatenate(
            [cache[pl.ds(at, size), head:] for at, size in pieces], axis=0
        )
        scores = lax.dot_general(
            query, keys, (((1,), (1,)), ((), ())), preferred_element_type=F32
        )
        own = jnp.sum(query.astype(F32) * key_new, axis=1, keepdims=True)
        def per_query(fact):
            return jnp.concatenate([fact[i, x]] * heads, axis=0)

        reach = per_query(lens)
        start = per_query(starts)
        offset = []
        for at, size in pieces:
            for n in range(size // TAIL):
                lane = lax.broadcasted_iota(jnp.int32, start.shape, 1)
                offset.append(lane + (at + n * TAIL) - start)
        reach = jnp.concatenate([reach] * len(offset), axis=1)
        offset = jnp.concatenate(offset, axis=1)
        usable = (offset >= 0) & (offset < reach)
        scores = jnp.where(usable, scores, NEGATIVE)
        top = jnp.maximum(jnp.max(scores, axis=1, keepdims=True), own)
        raw = jnp.where(usable, jnp.exp(scores - top), 0.0)
        raw_own = jnp.exp(own - top)
        total = jnp.sum(raw, axis=1, keepdims=True) + raw_own
        inverse = 1.0 / total
        weights = (raw * inverse).astype(BF16)
        own_weight = (raw_own * inverse).astype(BF16).astype(F32)
        attended = jnp.dot(weights, values, preferred_element_type=F32)
        attended = attended + own_weight * value_new
        att[i, x] = jnp.concatenate(
            [attended[h * group : (h + 1) * group] for h in range(heads)], axis=1
        ).astype(BF16)
        for d in (2, 1, 3):
            ag_copy(i, d).start()

    def update(i):
        for d in (1, 3, 2):
            ag_arrival(i, d).wait_recv()
        attended = att[i].astype(F32).reshape(rows, query_width).astype(BF16)
        depth = exits[i].reshape(rows, TAIL)
        final = ((y == last) & (i < DEEP)) | (i >= DEEP)
        active = jnp.concatenate([depth] * (span // TAIL), axis=1) > y
        for j in range(layers):

            @pl.when(i == 0)
            def _():
                wo_copies[j].wait()

            state = inb[i, j].astype(F32).reshape(rows, span)
            branch = jnp.dot(attended, wo[j], preferred_element_type=F32)
            updated = jnp.where(active, state + branch, state)
            updated = updated.reshape(shards, group, span).astype(BF16)
            outb[i, j] = updated

            @pl.when((y < last) & (i < DEEP))
            def _():
                state_copy(i, j).start()

            @pl.when(final & (y != j))
            def _():
                result_copy(i, j).start()

            @pl.when(final & (y == j))
            def _():
                settled[i] = updated

    def step(i, carry):
        @pl.when((y == 0) & (i == MAIN))
        def _():
            gather_late()

        @pl.when(i < count)
        def _():
            project(i)

        @pl.when((i >= LAG_A) & (i < count + LAG_A))
        def _():
            attend(i - LAG_A)

        @pl.when(i >= LAG_U)
        def _():
            update(i - LAG_U)

        return carry

    lax.fori_loop(0, count + LAG_U, step, 0)

    def arrive(i, carry):
        @pl.when(((y != last) & (i < DEEP)) | ((y != 0) & (i >= DEEP)))
        def _():
            result_copy(i, 0).wait_recv()

        return carry

    lax.fori_loop(0, TOTAL, arrive, 0)

    reach = lax.broadcasted_iota(jnp.int32, wide, 1)
    extra = settled[MAIN].astype(F32).reshape(rows, span)
    extra = jnp.concatenate([extra] + [jnp.zeros_like(extra)] * (SORTED - 1), axis=0)
    extra = extra.astype(BF16)
    for p in range(layers):
        found = jnp.concatenate(
            [
                settled[POSITION[p][c]].astype(F32).reshape(rows, span)
                for c in range(SORTED)
            ],
            axis=0,
        ).astype(BF16)
        goal = target[p]
        result = jnp.dot(
            number(goal == reach).astype(BF16), found, preferred_element_type=F32
        ) + jnp.dot(
            number(goal == reach + TAIL).astype(BF16), extra, preferred_element_type=F32
        )
        result = result.astype(BF16)
        out[p * BLOCK : (p + 1) * BLOCK, :] = result[:BLOCK]
        out[(p + layers) * BLOCK : (p + layers + 1) * BLOCK, :] = result[BLOCK:]

    def finish(i, carry):
        for d in range(1, shards):
            rs_copy(i, d).wait_send()
            ag_copy(i, d).wait_send()
        final = ((y == last) & (i < DEEP)) | (i >= DEEP)
        for j in range(layers):

            @pl.when((y < last) & (i < DEEP))
            def _():
                state_copy(i, j).wait_send()

            @pl.when(final & (y != j))
            def _():
                result_copy(i, j).wait_send()

        return carry

    lax.fori_loop(0, count, finish, 0)

    for p in (1, 3):

        @pl.when(y == layers - p)
        def _():
            hidden_sent(p, (2, 3))

    @pl.when(y == 2)
    def _():
        hidden_sent(2, (0, 1, 2, 3))


def full(shards, layers, hidden, gain, proj_weight, out_weight, cache, exits, lens):
    tokens = exits.shape[0] * exits.shape[1]
    quarter, width = proj_weight.shape
    query_width = out_weight.shape[0]
    span = quarter // layers
    group = BLOCK // shards // PARTS
    hidden = hidden.reshape(MICRO // layers, shards, PARTS, group, quarter)
    anywhere = pl.BlockSpec(memory_space=pl.ANY)
    vmem = pl.BlockSpec(memory_space=pltpu.VMEM)
    dma = pltpu.SemaphoreType.DMA
    column = (MICRO, shards, PARTS, group, TAIL)
    settled = pl.pallas_call(
        functools.partial(full_kernel, shards, layers),
        out_shape=jax.ShapeDtypeStruct((MICRO, shards, PARTS, group, span), BF16),
        in_specs=[anywhere, vmem, anywhere, anywhere, anywhere, vmem, vmem],
        out_specs=vmem,
        scratch_shapes=[
            pltpu.VMEM((layers, span, width), BF16),
            pltpu.VMEM((layers, query_width, span), BF16),
            pltpu.VMEM(cache.shape, BF16),
            pltpu.VMEM((CHUNKS, layers, shards, group, span), BF16),
            pltpu.VMEM((CHUNKS, layers, shards, group, span), BF16),
            pltpu.VMEM(column, jnp.int32),
            pltpu.VMEM(column, jnp.int32),
            pltpu.VMEM((CHUNKS, shards, group, width + TAIL), F32),
            pltpu.VMEM((CHUNKS, shards, group, width + TAIL), BF16),
            pltpu.VMEM((CHUNKS, shards, group, width + TAIL), BF16),
            pltpu.VMEM((CHUNKS, shards, group, query_width), BF16),
            dma((2 * layers + 1,)),
            dma((MICRO // layers, PARTS, layers)),
            dma((CHUNKS, layers)),
            dma((CHUNKS, shards - 1)),
            dma((CHUNKS, shards)),
            dma((CHUNKS, shards - 1)),
            dma((CHUNKS, shards)),
            dma((CHUNKS, layers)),
            dma((CHUNKS,)),
        ],
        compiler_params=pltpu.CompilerParams(
            collective_id=0, has_side_effects=True, vmem_limit_bytes=56 << 20
        ),
    )(hidden, gain, proj_weight, out_weight, cache, exits, lens)
    return settled.reshape(tokens, span)


def early(shards, layers, hidden, gain, proj_weight, out_weight, cache, exits, lens):
    tokens = exits.shape[0] * exits.shape[1]
    quarter, width = proj_weight.shape
    query_width = out_weight.shape[0]
    span = quarter // layers
    group = BLOCK // shards // PARTS
    rows = shards * group
    anywhere = pl.BlockSpec(memory_space=pl.ANY)
    vmem = pl.BlockSpec(memory_space=pltpu.VMEM)
    dma = pltpu.SemaphoreType.DMA
    fact = (TOTAL, shards, group, TAIL)
    return pl.pallas_call(
        functools.partial(early_kernel, shards, layers),
        out_shape=jax.ShapeDtypeStruct((tokens, span), BF16),
        in_specs=[anywhere, vmem, anywhere, anywhere, anywhere, vmem, vmem],
        out_specs=vmem,
        scratch_shapes=[
            pltpu.VMEM((layers, span, width), BF16),
            pltpu.VMEM((layers, query_width, span), BF16),
            pltpu.VMEM(cache.shape, BF16),
            pltpu.VMEM((TOTAL, layers, shards, group, span), BF16),
            pltpu.VMEM((TOTAL, layers, shards, group, span), BF16),
            pltpu.VMEM(hidden.shape, BF16),
            pltpu.VMEM((SORTED, layers, shards, group, span), BF16),
            pltpu.VMEM((TAIL, TAIL), BF16),
            pltpu.VMEM((layers, rows, TAIL), BF16),
            pltpu.VMEM((layers, TAIL, TAIL), jnp.int32),
            pltpu.VMEM((TOTAL, shards, group, span), BF16),
            pltpu.VMEM(fact, jnp.int32),
            pltpu.VMEM(fact, jnp.int32),
            pltpu.VMEM(fact, jnp.int32),
            pltpu.VMEM((TOTAL, shards, group, width + TAIL), F32),
            pltpu.VMEM((TOTAL, shards, group, width + TAIL), BF16),
            pltpu.VMEM((TOTAL, shards, group, width + TAIL), BF16),
            pltpu.VMEM((TOTAL, shards, group, query_width), BF16),
            dma((2 * layers + 1,)),
            dma((1,)),
            dma((SORTED, layers)),
            pltpu.SemaphoreType.REGULAR,
            dma((TOTAL, layers)),
            dma((TOTAL, shards - 1)),
            dma((TOTAL, shards)),
            dma((TOTAL, shards - 1)),
            dma((TOTAL, shards)),
            dma((TOTAL, layers)),
            dma((TOTAL,)),
        ],
        compiler_params=pltpu.CompilerParams(
            collective_id=1, has_side_effects=True, vmem_limit_bytes=56 << 20
        ),
    )(hidden, gain, proj_weight, out_weight, cache, exits, lens)


def body(hidden, exit_layer, lengths, kv_cache, norm_gain, w_qkv, w_out):
    devices = lax.axis_size("section")
    shards = max(2, devices // 4)
    layers = devices // shards
    tokens = exit_layer.shape[0]
    cache = kv_cache.reshape(kv_cache.shape[1] * kv_cache.shape[2], kv_cache.shape[3])
    exits = exit_layer.reshape(tokens // TAIL, TAIL)
    lens = lengths.reshape(tokens // TAIL, TAIL)
    operands = (hidden[0], norm_gain, w_qkv[0], w_out[0], cache, exits, lens)
    going = (exit_layer > 1).astype(jnp.int32)
    going = going.reshape(MICRO // layers, layers, shards, BLOCK // shards)
    over = jnp.maximum(jnp.sum(going, axis=(0, 3)) - KEEP, 0)
    fits = jnp.max(jnp.sum(over, axis=0)) <= BLOCK // shards // PARTS
    return lax.cond(
        fits,
        functools.partial(early, shards, layers),
        functools.partial(full, shards, layers),
        *operands,
    )


def solution(mesh):
    return jax.shard_map(
        body,
        mesh=mesh,
        in_specs=(
            P("section", "blk", None),
            P("blk"),
            P("blk"),
            P("section", "blk", None, None),
            P("section", None),
            P("section", None, None),
            P("section", None, None),
        ),
        out_specs=P("blk", "section"),
        check_vma=False,
    )
```

```python
import functools
import math

import jax
import jax.numpy as jnp
from jax import lax
from jax.experimental import pallas as pl
from jax.experimental.pallas import tpu as pltpu
from jax.sharding import PartitionSpec as P

BLOCK = 64
MICRO = 8
PARTS = 2
CHUNKS = MICRO * PARTS
CONTEXT = 16
SORTED = 4
FIRST = 8
KEEP = 16
POSITION = ((0, 1, 10, 11), (3, 7, 13, 16), (4, 8, 14, 17), (2, 6, 12, 15))
GATHERED = (5, 9)
DEEPEST = 6
DEEP = 10
TOTAL = 18
LAG_A = 1
LAG_U = 2
EPSILON = 1e-05
NEGATIVE = -1e30
TAIL = 128
MESH = pl.DeviceIdType.MESH
F32 = jnp.float32
BF16 = jnp.bfloat16


def full_kernel(
    shards,
    layers,
    hidden,
    gain,
    wq_hbm,
    wo_hbm,
    cache_hbm,
    exit_rows,
    length_rows,
    out,
    wq,
    wo,
    cache,
    inb,
    outb,
    exits,
    lens,
    accs,
    rs_send,
    rs_recv,
    att,
    w_sem,
    hid_ss,
    in_rs,
    rs_ss,
    rs_rs,
    ag_ss,
    ag_rs,
    st_ss,
    out_rs,
):
    me = lax.axis_index("section")
    y = me // shards
    x = me % shards
    last = layers - 1
    group, span = inb.shape[3:]
    rows = shards * group
    query_width = wo.shape[1]
    width = wq.shape[2]
    head = (width - query_width) // 2
    heads = query_width // head
    context = cache.shape[0] // (CHUNKS * group)
    total_width = span * shards * layers

    def remote(src, dst, send_sem, recv_sem, target):
        return pltpu.make_async_remote_copy(
            src_ref=src,
            dst_ref=dst,
            send_sem=send_sem,
            recv_sem=recv_sem,
            device_id={"section": target},
            device_id_type=MESH,
        )

    def row_peer(d):
        return y * shards + (x + d) % shards

    wq_copies = [
        pltpu.make_async_copy(wq_hbm.at[pl.ds(j * span, span)], wq.at[j], w_sem.at[j])
        for j in range(layers)
    ]
    wo_copies = [
        pltpu.make_async_copy(
            wo_hbm.at[:, pl.ds(j * span, span)], wo.at[j], w_sem.at[layers + j]
        )
        for j in range(layers)
    ]
    cache_copy = pltpu.make_async_copy(cache_hbm, cache, w_sem.at[2 * layers])
    for copy in wq_copies:
        copy.start()
    cache_copy.start()
    for copy in wo_copies:
        copy.start()

    barrier = pltpu.get_barrier_semaphore()
    for d in range(1, shards):
        pl.semaphore_signal(
            barrier, inc=1, device_id={"section": row_peer(d)}, device_id_type=MESH
        )
    for d in range(1, layers):
        pl.semaphore_signal(
            barrier,
            inc=1,
            device_id={"section": ((y + d) % layers) * shards + x},
            device_id_type=MESH,
        )
    pl.semaphore_wait(barrier, shards + layers - 2)

    rounds = MICRO // layers
    place = (layers - y) % layers

    pieces = [
        (q, h, j) for q in range(rounds) for h in range(PARTS) for j in range(layers)
    ]

    def hidden_piece(q, h, j):
        return hidden.at[q, :, h, :, pl.ds(j * span, span)]

    def hidden_copy(q, h, j):
        i = (q * layers + place) * PARTS + h
        return remote(
            hidden_piece(q, h, j), inb.at[i, j], hid_ss.at[q, h, j], in_rs.at[i, j], x
        )

    @pl.when(y == 0)
    def _():
        for q, h, j in pieces:
            i = q * layers * PARTS + h
            pltpu.make_async_copy(
                hidden_piece(q, h, j), inb.at[i, j], in_rs.at[i, j]
            ).start()

    @pl.when(y != 0)
    def _():
        for q, h, j in pieces:
            hidden_copy(q, h, j).start()

    for r in range(exit_rows.shape[0]):
        for source, target in ((exit_rows, exits), (length_rows, lens)):
            spread = jnp.broadcast_to(source[r : r + 1, :], (TAIL, TAIL)).T
            count = TAIL // BLOCK
            target[r * count : (r + 1) * count] = spread.reshape(
                (count,) + target.shape[1:]
            )

    def rs_copy(i, d):
        target = (x + d) % shards
        return remote(
            rs_send.at[i, target],
            rs_recv.at[i, x],
            rs_ss.at[i, d - 1],
            rs_rs.at[i, x],
            row_peer(d),
        )

    def rs_arrival(i, d):
        source = (x + d) % shards
        return remote(
            rs_send.at[i, source],
            rs_recv.at[i, source],
            rs_ss.at[i, d - 1],
            rs_rs.at[i, source],
            row_peer(d),
        )

    def ag_copy(i, d):
        return remote(
            att.at[i, x], att.at[i, x], ag_ss.at[i, d - 1], ag_rs.at[i, x], row_peer(d)
        )

    def ag_arrival(i, d):
        source = (x + d) % shards
        return remote(
            att.at[i, source],
            att.at[i, source],
            ag_ss.at[i, d - 1],
            ag_rs.at[i, source],
            row_peer(d),
        )

    def state_copy(i, j):
        return remote(
            outb.at[i, j],
            inb.at[i, j],
            st_ss.at[i, j],
            in_rs.at[i, j],
            (me + shards) % (shards * layers),
        )

    def tokens(ref, i):
        return ref.at[i // PARTS, :, i % PARTS]

    def result_copy(i, j):
        return remote(
            outb.at[i, j], tokens(out, i), st_ss.at[i, j], out_rs.at[i], j * shards + x
        )

    def project(i):
        squares = jnp.zeros((rows, TAIL), F32)
        acc = None
        for j in range(layers):

            @pl.when(i == 0)
            def _():
                wq_copies[j].wait()

            state_copy(i, j).wait_recv()
            state = inb[i, j].astype(F32).reshape(rows, span)
            scaled = (state * gain[:, pl.ds(j * span, span)].astype(F32)).astype(BF16)
            squared = state * state
            for n in range(span // TAIL):
                squares = squares + squared[:, n * TAIL : (n + 1) * TAIL]
            part = jnp.dot(scaled, wq[j], preferred_element_type=F32)
            acc = part if acc is None else acc + part
        total = jnp.sum(squares, axis=1, keepdims=True)
        coarse = total.astype(BF16).astype(F32)
        lane = lax.broadcasted_iota(jnp.int32, (rows, TAIL), 1)
        tail = jnp.where(lane < TAIL // 2, coarse, total - coarse)
        for g in range(shards):
            part = slice(g * group, (g + 1) * group)
            accs[i, g, :, :width] = acc[part]
            accs[i, g, :, width:] = tail[part]
            rs_send[i, g, :, :width] = acc[part].astype(BF16)
            rs_send[i, g, :, width:] = tail[part].astype(BF16)
        for d in (2, 1, 3):
            rs_copy(i, d).start()

    def attend(i):
        @pl.when(i == 0)
        def _():
            cache_copy.wait()

        summed = accs[i, x]
        for d in (1, 3, 2):
            rs_arrival(i, d).wait_recv()
        for d in (1, 3, 2):
            summed = summed + rs_recv[i, (x + d) % shards].astype(F32)
        squares = jnp.sum(summed[:, width:], axis=1, keepdims=True) * (2.0 / TAIL)
        scale = lax.rsqrt(squares / total_width + EPSILON)
        fitted = summed[:, :width] * scale
        query = fitted[:, :query_width] * (1.0 / math.sqrt(head))
        query = jnp.concatenate(
            [query[:, h * head : (h + 1) * head] for h in range(heads)], axis=0
        ).astype(BF16)
        key_new = fitted[:, query_width : query_width + head].astype(BF16).astype(F32)
        value_new = fitted[:, query_width + head :].astype(BF16).astype(F32)
        key_new = jnp.concatenate([key_new] * heads, axis=0)
        value_new = jnp.concatenate([value_new] * heads, axis=0)
        held = group * context
        keys = cache[pl.ds(pl.multiple_of(i * held, held), held), :head]
        values = cache[pl.ds(pl.multiple_of(i * held, held), held), head:]
        scores = lax.dot_general(
            query, keys, (((1,), (1,)), ((), ())), preferred_element_type=F32
        )
        own = jnp.sum(query.astype(F32) * key_new, axis=1, keepdims=True)
        reach = lens[i // PARTS, x, i % PARTS]
        reach = jnp.concatenate([reach] * (held // TAIL), axis=1)
        reach = jnp.concatenate([reach] * heads, axis=0)
        shape = (heads * group, held)
        row = lax.broadcasted_iota(jnp.int32, shape, 0)
        column = lax.broadcasted_iota(jnp.int32, shape, 1)
        offset = column - (row % group) * context
        usable = (offset >= 0) & (offset < reach)
        scores = jnp.where(usable, scores, NEGATIVE)
        top = jnp.maximum(jnp.max(scores, axis=1, keepdims=True), own)
        raw = jnp.where(usable, jnp.exp(scores - top), 0.0)
        raw_own = jnp.exp(own - top)
        total = jnp.sum(raw, axis=1, keepdims=True) + raw_own
        inverse = 1.0 / total
        weights = (raw * inverse).astype(BF16)
        own_weight = (raw_own * inverse).astype(BF16).astype(F32)
        attended = jnp.dot(weights, values, preferred_element_type=F32)
        attended = attended + own_weight * value_new
        att[i, x] = jnp.concatenate(
            [attended[h * group : (h + 1) * group] for h in range(heads)], axis=1
        ).astype(BF16)
        for d in (2, 1, 3):
            ag_copy(i, d).start()

    def update(i):
        for d in (1, 3, 2):
            ag_arrival(i, d).wait_recv()
        attended = att[i].astype(F32).reshape(rows, query_width).astype(BF16)
        depth = exits[i // PARTS, :, i % PARTS].reshape(rows, TAIL)
        active = jnp.concatenate([depth] * (span // TAIL), axis=1) > y
        for j in range(layers):

            @pl.when(i == 0)
            def _():
                wo_copies[j].wait()

            state = inb[i, j].astype(F32).reshape(rows, span)
            branch = jnp.dot(attended, wo[j], preferred_element_type=F32)
            updated = jnp.where(active, state + branch, state)
            updated = updated.reshape(shards, group, span).astype(BF16)
            outb[i, j] = updated

            @pl.when(y < last)
            def _():
                state_copy(i, j).start()

            if j < last:

                @pl.when(y == last)
                def _():
                    result_copy(i, j).start()

            else:

                @pl.when(y == last)
                def _():
                    out[i // PARTS, :, i % PARTS] = updated

    def step(i, carry):
        @pl.when(i < CHUNKS)
        def _():
            project(i)

        @pl.when((i >= LAG_A) & (i < CHUNKS + LAG_A))
        def _():
            attend(i - LAG_A)

        @pl.when(i >= LAG_U)
        def _():
            update(i - LAG_U)

        return carry

    lax.fori_loop(0, CHUNKS + LAG_U, step, 0)

    def finish(i, carry):
        for d in range(1, shards):
            rs_copy(i, d).wait_send()
            ag_copy(i, d).wait_send()
        for j in range(layers):

            @pl.when(y < last)
            def _():
                state_copy(i, j).wait_send()

            if j < last:

                @pl.when(y == last)
                def _():
                    result_copy(i, j).wait_send()

        @pl.when(y < last)
        def _():
            result_copy(i, 0).wait_recv()

        return carry

    lax.fori_loop(0, CHUNKS, finish, 0)

    @pl.when(y != 0)
    def _():
        for q, h, j in pieces:
            hidden_copy(q, h, j).wait_send()


def early_kernel(
    shards,
    layers,
    hidden,
    gain,
    wq_hbm,
    wo_hbm,
    cache_hbm,
    exit_rows,
    length_rows,
    out,
    wq,
    wo,
    cache,
    inb,
    outb,
    hid,
    staged,
    late_pick,
    target,
    settled,
    exits,
    lens,
    starts,
    accs,
    rs_send,
    rs_recv,
    att,
    w_sem,
    hid_in,
    hid_ss,
    turn,
    in_rs,
    rs_ss,
    rs_rs,
    ag_ss,
    ag_rs,
    st_ss,
    out_rs,
):
    me = lax.axis_index("section")
    y = me // shards
    x = me % shards
    last = layers - 1
    group, span = inb.shape[3:]
    rows = shards * group
    query_width = wo.shape[1]
    width = wq.shape[2]
    head = (width - query_width) // 2
    heads = query_width // head
    context = CONTEXT
    passing = DEEP - (DEEP - DEEPEST) * (y // (last - 1))
    count = (
        DEEP
        + (TOTAL - DEEP) * ((last - y) // last)
        - (DEEP - DEEPEST) * (y // last)
    )
    total_width = span * shards * layers

    def remote(src, dst, send_sem, recv_sem, target):
        return pltpu.make_async_remote_copy(
            src_ref=src,
            dst_ref=dst,
            send_sem=send_sem,
            recv_sem=recv_sem,
            device_id={"section": target},
            device_id_type=MESH,
        )

    def row_peer(d):
        return y * shards + (x + d) % shards

    wq_copies = [
        pltpu.make_async_copy(wq_hbm.at[pl.ds(j * span, span)], wq.at[j], w_sem.at[j])
        for j in range(layers)
    ]
    wo_copies = [
        pltpu.make_async_copy(
            wo_hbm.at[:, pl.ds(j * span, span)], wo.at[j], w_sem.at[layers + j]
        )
        for j in range(layers)
    ]
    cache_copy = pltpu.make_async_copy(cache_hbm, cache, w_sem.at[2 * layers])
    hid_copy = pltpu.make_async_copy(hidden, hid, hid_in.at[0])
    hid_copy.start()
    for copy in wq_copies:
        copy.start()
    cache_copy.start()
    for copy in wo_copies:
        copy.start()

    barrier = pltpu.get_barrier_semaphore()
    for d in range(1, shards):
        pl.semaphore_signal(
            barrier, inc=1, device_id={"section": row_peer(d)}, device_id_type=MESH
        )
    for d in range(1, layers):
        pl.semaphore_signal(
            barrier,
            inc=1,
            device_id={"section": ((y + d) % layers) * shards + x},
            device_id_type=MESH,
        )

    wide = (TAIL, TAIL)
    t0 = lax.broadcasted_iota(jnp.int32, wide, 0)
    t1 = lax.broadcasted_iota(jnp.int32, wide, 1)
    g0 = (t0 & (BLOCK - 1)) >> 4
    g1 = (t1 & (BLOCK - 1)) >> 4
    same = g0 == g1
    lane_group = (t1 & 31) >> 3
    lane_rank = ((t1 >> 5) << 3) + (t1 & 7)
    slot_row = lax.broadcasted_iota(jnp.int32, (rows, TAIL), 0)
    low_half = t1 < BLOCK
    def number(mask):
        return jnp.where(mask, 1.0, 0.0)

    def piece_row(ref, p):
        first = jnp.broadcast_to(ref[pl.ds(p // 2, 1), :], wide)
        second = jnp.broadcast_to(ref[pl.ds(p // 2 + 2, 1), :], wide)
        even = jnp.where(low_half, first, pltpu.roll(second, BLOCK, 1))
        odd = jnp.where(low_half, pltpu.roll(first, BLOCK, 1), second)
        if isinstance(p, int):
            return odd if p % 2 else even
        parity = p % 2
        return even * (1 - parity) + odd * parity

    def rank_of(exit_row, exit_column):
        ahead = same & (
            (exit_column > exit_row) | ((exit_column == exit_row) & (t0 < t1))
        )
        rank_lane = jnp.sum(number(ahead), axis=0, keepdims=True).astype(jnp.int32)
        order_lane = ((rank_lane >> 3) << 5) + (g1 << 3) + (rank_lane & 7)
        return number(order_lane == t0).astype(BF16)

    own_row = piece_row(exit_rows, (layers - y) % layers)
    own_pick = rank_of(own_row, own_row.T)

    hid_copy.wait()
    for j in range(layers):
        ordered = jnp.dot(
            own_pick,
            hid[:, j * span : (j + 1) * span],
            preferred_element_type=F32,
        )
        ordered = ordered.reshape(SORTED, shards, group, span).astype(BF16)

        @pl.when(y == 0)
        def _():
            for c in range(SORTED):
                inb[POSITION[0][c], j] = ordered[c]

        @pl.when(y != 0)
        def _():
            for c in range(SORTED):
                staged[c, j] = ordered[c]

    pl.semaphore_wait(barrier, shards + layers - 2)

    def hidden_copy(p, c, j):
        i = POSITION[p][c]
        return remote(
            staged.at[c, j], inb.at[i, j], hid_ss.at[c, j], in_rs.at[i, j], x
        )

    def hidden_start(p, c):
        for j in range(layers):
            hidden_copy(p, c, j).start()

    def hidden_sent(p, c, pieces):
        for j in pieces:
            hidden_copy(p, c, j).wait_send()

    every = range(layers)

    def next_turn():
        pl.semaphore_signal(
            turn, inc=1, device_id={"section": me - shards}, device_id_type=MESH
        )

    @pl.when(y == 1)
    def _():
        for c in range(2):
            hidden_start(3, c)
            hidden_sent(3, c, every)
        for c in range(2, SORTED):
            hidden_start(3, c)

    @pl.when(y == 2)
    def _():
        for c in range(2):
            pl.semaphore_wait(turn, 1)
            hidden_start(2, c)
        pl.semaphore_wait(turn, 1)
        for c in range(2, SORTED):
            hidden_start(2, c)

    @pl.when(y == 3)
    def _():
        hidden_start(1, 0)
        hidden_sent(1, 0, every[:2])
        next_turn()
        hidden_sent(1, 0, every[2:])
        hidden_start(1, 1)
        hidden_sent(1, 1, every[:1])
        next_turn()
        hidden_sent(1, 1, every[1:])
        next_turn()
        for c in range(2, SORTED):
            hidden_start(1, c)

    def prepare():
        kinds = ((FIRST, last), (KEEP, 1))
        base_lane = [jnp.zeros((1, TAIL), jnp.int32) for _ in kinds]
        base_column = [jnp.zeros((TAIL, 1), jnp.int32) for _ in kinds]
        late = [jnp.zeros((rows, 3 * TAIL), F32) for _ in kinds]

        for p in range(layers):
            exit_row = piece_row(exit_rows, p)
            exit_column = exit_row.T
            length_column = piece_row(length_rows, p).T
            pick = rank_of(exit_row, exit_column)
            behind = same & (
                (exit_row > exit_column) | ((exit_row == exit_column) & (t1 < t0))
            )
            rank_column = jnp.sum(number(behind), axis=1, keepdims=True).astype(jnp.int32)
            order_column = ((rank_column >> 3) << 5) + (g0 << 3) + (rank_column & 7)
            natural = ((p + layers * (t0 >> 6)) << 4) + (t0 & 15)
            facts = jnp.concatenate([exit_column, length_column, natural], axis=1)
            sorted_facts = jnp.dot(
                pick, facts.astype(F32).astype(BF16), preferred_element_type=F32
            )
            for c in range(SORTED):
                block = sorted_facts[c * rows : (c + 1) * rows].astype(jnp.int32)
                block = block.reshape(shards, group, 3 * TAIL)
                exits[POSITION[p][c]] = block[:, :, :TAIL]
                lens[POSITION[p][c]] = block[:, :, TAIL : 2 * TAIL]
                starts[POSITION[p][c]] = block[:, :, 2 * TAIL :] * context
            goal = order_column
            for n, (first, depth) in reversed(list(enumerate(kinds))):
                deep_column = jnp.sum(
                    number(same & (exit_row > depth)), axis=1, keepdims=True
                ).astype(jnp.int32)
                deep_lane = jnp.sum(
                    number((exit_column > depth) & (g0 == lane_group)), axis=0, keepdims=True
                ).astype(jnp.int32)
                ranked = lane_rank[:rows]
                chosen = (
                    (ranked >= first)
                    & (ranked < deep_lane)
                    & (lane_group[:rows] == (slot_row >> 3))
                    & (base_lane[n] + ranked - first == (slot_row & 7))
                )
                chosen = number(chosen).astype(BF16)
                late_pick[n, p] = chosen
                late[n] = late[n] + jnp.dot(
                    chosen, sorted_facts.astype(BF16), preferred_element_type=F32
                )
                goal = jnp.where(
                    (rank_column >= first) & (rank_column < deep_column),
                    TAIL + n * rows + (g0 << 3) + base_column[n] + rank_column - first,
                    goal,
                )
                base_lane[n] = base_lane[n] + jnp.maximum(deep_lane - first, 0)
                base_column[n] = base_column[n] + jnp.maximum(deep_column - first, 0)
            target[p] = goal
        for n, i in enumerate(GATHERED):
            block = late[n].astype(jnp.int32).reshape(shards, group, 3 * TAIL)
            exits[i] = block[:, :, :TAIL]
            lens[i] = block[:, :, TAIL : 2 * TAIL]
            starts[i] = block[:, :, 2 * TAIL :] * context

    def rs_copy(i, d):
        target = (x + d) % shards
        return remote(
            rs_send.at[i, target],
            rs_recv.at[i, x],
            rs_ss.at[i, d - 1],
            rs_rs.at[i, x],
            row_peer(d),
        )

    def rs_arrival(i, d):
        source = (x + d) % shards
        return remote(
            rs_send.at[i, source],
            rs_recv.at[i, source],
            rs_ss.at[i, d - 1],
            rs_rs.at[i, source],
            row_peer(d),
        )

    def ag_copy(i, d):
        return remote(
            att.at[i, x], att.at[i, x], ag_ss.at[i, d - 1], ag_rs.at[i, x], row_peer(d)
        )

    def ag_arrival(i, d):
        source = (x + d) % shards
        return remote(
            att.at[i, source],
            att.at[i, source],
            ag_ss.at[i, d - 1],
            ag_rs.at[i, source],
            row_peer(d),
        )

    def state_copy(i, j):
        return remote(
            outb.at[i, j],
            inb.at[i, j],
            st_ss.at[i, j],
            in_rs.at[i, j],
            (me + shards) % (shards * layers),
        )

    def result_copy(i, j):
        return remote(
            outb.at[i, j], settled.at[i], st_ss.at[i, j], out_rs.at[i], j * shards + x
        )

    def gather_late(n, chunks):
        for c in chunks:
            for p in range(1, layers):
                for j in range(layers):
                    state_copy(POSITION[p][c], j).wait_recv()
        for j in range(layers):
            found = None
            for p in range(layers):
                held = [
                    inb[POSITION[p][c], j].astype(F32).reshape(rows, span)
                    if c in chunks
                    else jnp.zeros((rows, span), F32)
                    for c in range(SORTED)
                ]
                held = jnp.concatenate(held, axis=0).astype(BF16)
                part = jnp.dot(late_pick[n, p], held, preferred_element_type=F32)
                found = part if found is None else found + part
            inb[GATHERED[n], j] = found.reshape(shards, group, span).astype(BF16)

    def project(i):
        squares = jnp.zeros((rows, TAIL), F32)
        acc = None
        for j in range(layers):

            @pl.when(i == 0)
            def _():
                wq_copies[j].wait()

            @pl.when((y > 0) | ((i > 1) & (i < GATHERED[0])))
            def _():
                state_copy(i, j).wait_recv()

            state = inb[i, j].astype(F32).reshape(rows, span)
            scaled = (state * gain[:, pl.ds(j * span, span)].astype(F32)).astype(BF16)
            squared = state * state
            for n in range(span // TAIL):
                squares = squares + squared[:, n * TAIL : (n + 1) * TAIL]
            part = jnp.dot(scaled, wq[j], preferred_element_type=F32)
            acc = part if acc is None else acc + part
        total = jnp.sum(squares, axis=1, keepdims=True)
        coarse = total.astype(BF16).astype(F32)
        lane = lax.broadcasted_iota(jnp.int32, (rows, TAIL), 1)
        tail = jnp.where(lane < TAIL // 2, coarse, total - coarse)
        for g in range(shards):
            part = slice(g * group, (g + 1) * group)
            accs[i, g, :, :width] = acc[part]
            accs[i, g, :, width:] = tail[part]
            rs_send[i, g, :, :width] = acc[part].astype(BF16)
            rs_send[i, g, :, width:] = tail[part].astype(BF16)
        for d in (2, 1, 3):
            rs_copy(i, d).start()

    def attend(i):
        @pl.when(i == 0)
        def _():
            cache_copy.wait()

        turn = (1 - i // DEEP) * ((i + 2) % layers) + (i // DEEP) * (i % last)
        p = ((i % DEEP + 8) // DEEP) * ((last - 2 * turn + last * (turn // 2)) % layers)
        half = shards * shards * context

        @pl.when((i == GATHERED[0]) | (i == GATHERED[1]))
        def _():
            attend_over(i, [(0, cache.shape[0])])

        @pl.when((i != GATHERED[0]) & (i != GATHERED[1]))
        def _():
            attend_over(
                i,
                [
                    (pl.multiple_of(p * half, half), half),
                    (pl.multiple_of((p + layers) * half, half), half),
                ],
            )

    def attend_over(i, pieces):

        summed = accs[i, x]
        for d in (1, 3, 2):
            rs_arrival(i, d).wait_recv()
        for d in (1, 3, 2):
            summed = summed + rs_recv[i, (x + d) % shards].astype(F32)
        squares = jnp.sum(summed[:, width:], axis=1, keepdims=True) * (2.0 / TAIL)
        scale = lax.rsqrt(squares / total_width + EPSILON)
        fitted = summed[:, :width] * scale
        query = fitted[:, :query_width] * (1.0 / math.sqrt(head))
        query = jnp.concatenate(
            [query[:, h * head : (h + 1) * head] for h in range(heads)], axis=0
        ).astype(BF16)
        key_new = fitted[:, query_width : query_width + head].astype(BF16).astype(F32)
        value_new = fitted[:, query_width + head :].astype(BF16).astype(F32)
        key_new = jnp.concatenate([key_new] * heads, axis=0)
        value_new = jnp.concatenate([value_new] * heads, axis=0)
        keys = jnp.concatenate(
            [cache[pl.ds(at, size), :head] for at, size in pieces], axis=0
        )
        values = jnp.concatenate(
            [cache[pl.ds(at, size), head:] for at, size in pieces], axis=0
        )
        scores = lax.dot_general(
            query, keys, (((1,), (1,)), ((), ())), preferred_element_type=F32
        )
        own = jnp.sum(query.astype(F32) * key_new, axis=1, keepdims=True)
        def per_query(fact):
            return jnp.concatenate([fact[i, x]] * heads, axis=0)

        reach = per_query(lens)
        start = per_query(starts)
        offset = []
        for at, size in pieces:
            for n in range(size // TAIL):
                lane = lax.broadcasted_iota(jnp.int32, start.shape, 1)
                offset.append(lane + (at + n * TAIL) - start)
        reach = jnp.concatenate([reach] * len(offset), axis=1)
        offset = jnp.concatenate(offset, axis=1)
        usable = (offset >= 0) & (offset < reach)
        scores = jnp.where(usable, scores, NEGATIVE)
        top = jnp.maximum(jnp.max(scores, axis=1, keepdims=True), own)
        raw = jnp.where(usable, jnp.exp(scores - top), 0.0)
        raw_own = jnp.exp(own - top)
        total = jnp.sum(raw, axis=1, keepdims=True) + raw_own
        inverse = 1.0 / total
        weights = (raw * inverse).astype(BF16)
        own_weight = (raw_own * inverse).astype(BF16).astype(F32)
        attended = jnp.dot(weights, values, preferred_element_type=F32)
        attended = attended + own_weight * value_new
        att[i, x] = jnp.concatenate(
            [attended[h * group : (h + 1) * group] for h in range(heads)], axis=1
        ).astype(BF16)
        for d in (2, 1, 3):
            ag_copy(i, d).start()

    def update(i):
        for d in (1, 3, 2):
            ag_arrival(i, d).wait_recv()
        attended = att[i].astype(F32).reshape(rows, query_width).astype(BF16)
        depth = exits[i].reshape(rows, TAIL)
        final = (y == last) | (i >= passing)
        active = jnp.concatenate([depth] * (span // TAIL), axis=1) > y
        for j in range(layers):

            @pl.when(i == 0)
            def _():
                wo_copies[j].wait()

            state = inb[i, j].astype(F32).reshape(rows, span)
            branch = jnp.dot(attended, wo[j], preferred_element_type=F32)
            updated = jnp.where(active, state + branch, state)
            updated = updated.reshape(shards, group, span).astype(BF16)
            outb[i, j] = updated

            @pl.when((y < last) & (i < passing))
            def _():
                state_copy(i, j).start()

            @pl.when(final & (y != j))
            def _():
                result_copy(i, j).start()

            @pl.when(final & (y == j))
            def _():
                settled[i] = updated

    def step(i, carry):
        @pl.when((y == 0) & (i == GATHERED[0]))
        def _():
            gather_late(0, (1,))

        @pl.when((y == 0) & (i == GATHERED[1]))
        def _():
            gather_late(1, (2, 3))

        @pl.when(i < count)
        def _():
            project(i)

        @pl.when(i == LAG_A)
        def _():
            prepare()

        @pl.when((i >= LAG_A) & (i < count + LAG_A))
        def _():
            attend(i - LAG_A)

        @pl.when(i >= LAG_U)
        def _():
            update(i - LAG_U)

        return carry

    lax.fori_loop(0, count + LAG_U, step, 0)

    def arrive(i, carry):
        @pl.when(
            ((y != last) & (i < DEEPEST))
            | ((y != last - 1) & (i >= DEEPEST) & (i < DEEP))
            | ((y != 0) & (i >= DEEP))
        )
        def _():
            result_copy(i, 0).wait_recv()

        return carry

    lax.fori_loop(0, TOTAL, arrive, 0)

    reach = lax.broadcasted_iota(jnp.int32, wide, 1)
    extra = [settled[i].astype(F32).reshape(rows, span) for i in GATHERED]
    extra = jnp.concatenate(extra + [jnp.zeros((2 * rows, span), F32)], axis=0)
    extra = extra.astype(BF16)
    for p in range(layers):
        found = jnp.concatenate(
            [
                settled[POSITION[p][c]].astype(F32).reshape(rows, span)
                for c in range(SORTED)
            ],
            axis=0,
        ).astype(BF16)
        goal = target[p]
        result = jnp.dot(
            number(goal == reach).astype(BF16), found, preferred_element_type=F32
        ) + jnp.dot(
            number(goal == reach + TAIL).astype(BF16), extra, preferred_element_type=F32
        )
        result = result.astype(BF16)
        out[p * BLOCK : (p + 1) * BLOCK, :] = result[:BLOCK]
        out[(p + layers) * BLOCK : (p + layers + 1) * BLOCK, :] = result[BLOCK:]

    def finish(i, carry):
        for d in range(1, shards):
            rs_copy(i, d).wait_send()
            ag_copy(i, d).wait_send()
        final = (y == last) | (i >= passing)
        for j in range(layers):

            @pl.when((y < last) & (i < passing))
            def _():
                state_copy(i, j).wait_send()

            @pl.when(final & (y != j))
            def _():
                result_copy(i, j).wait_send()

        return carry

    lax.fori_loop(0, count, finish, 0)

    for p in range(1, layers):

        @pl.when(y == layers - p)
        def _():
            for c in range(2, SORTED):
                hidden_sent(p, c, every)

    @pl.when(y == 2)
    def _():
        for c in range(2):
            hidden_sent(2, c, every)


def full(shards, layers, hidden, gain, proj_weight, out_weight, cache, exits, lens):
    tokens = exits.shape[0] * exits.shape[1]
    quarter, width = proj_weight.shape
    query_width = out_weight.shape[0]
    span = quarter // layers
    group = BLOCK // shards // PARTS
    hidden = hidden.reshape(MICRO // layers, shards, PARTS, group, quarter)
    anywhere = pl.BlockSpec(memory_space=pl.ANY)
    vmem = pl.BlockSpec(memory_space=pltpu.VMEM)
    dma = pltpu.SemaphoreType.DMA
    column = (MICRO, shards, PARTS, group, TAIL)
    settled = pl.pallas_call(
        functools.partial(full_kernel, shards, layers),
        out_shape=jax.ShapeDtypeStruct((MICRO, shards, PARTS, group, span), BF16),
        in_specs=[anywhere, vmem, anywhere, anywhere, anywhere, vmem, vmem],
        out_specs=vmem,
        scratch_shapes=[
            pltpu.VMEM((layers, span, width), BF16),
            pltpu.VMEM((layers, query_width, span), BF16),
            pltpu.VMEM(cache.shape, BF16),
            pltpu.VMEM((CHUNKS, layers, shards, group, span), BF16),
            pltpu.VMEM((CHUNKS, layers, shards, group, span), BF16),
            pltpu.VMEM(column, jnp.int32),
            pltpu.VMEM(column, jnp.int32),
            pltpu.VMEM((CHUNKS, shards, group, width + TAIL), F32),
            pltpu.VMEM((CHUNKS, shards, group, width + TAIL), BF16),
            pltpu.VMEM((CHUNKS, shards, group, width + TAIL), BF16),
            pltpu.VMEM((CHUNKS, shards, group, query_width), BF16),
            dma((2 * layers + 1,)),
            dma((MICRO // layers, PARTS, layers)),
            dma((CHUNKS, layers)),
            dma((CHUNKS, shards - 1)),
            dma((CHUNKS, shards)),
            dma((CHUNKS, shards - 1)),
            dma((CHUNKS, shards)),
            dma((CHUNKS, layers)),
            dma((CHUNKS,)),
        ],
        compiler_params=pltpu.CompilerParams(
            collective_id=0, has_side_effects=True, vmem_limit_bytes=56 << 20
        ),
    )(hidden, gain, proj_weight, out_weight, cache, exits, lens)
    return settled.reshape(tokens, span)


def early(shards, layers, hidden, gain, proj_weight, out_weight, cache, exits, lens):
    tokens = exits.shape[0] * exits.shape[1]
    quarter, width = proj_weight.shape
    query_width = out_weight.shape[0]
    span = quarter // layers
    group = BLOCK // shards // PARTS
    rows = shards * group
    anywhere = pl.BlockSpec(memory_space=pl.ANY)
    vmem = pl.BlockSpec(memory_space=pltpu.VMEM)
    dma = pltpu.SemaphoreType.DMA
    fact = (TOTAL, shards, group, TAIL)
    return pl.pallas_call(
        functools.partial(early_kernel, shards, layers),
        out_shape=jax.ShapeDtypeStruct((tokens, span), BF16),
        in_specs=[anywhere, vmem, anywhere, anywhere, anywhere, vmem, vmem],
        out_specs=vmem,
        scratch_shapes=[
            pltpu.VMEM((layers, span, width), BF16),
            pltpu.VMEM((layers, query_width, span), BF16),
            pltpu.VMEM(cache.shape, BF16),
            pltpu.VMEM((TOTAL, layers, shards, group, span), BF16),
            pltpu.VMEM((TOTAL, layers, shards, group, span), BF16),
            pltpu.VMEM(hidden.shape, BF16),
            pltpu.VMEM((SORTED, layers, shards, group, span), BF16),
            pltpu.VMEM((2, layers, rows, TAIL), BF16),
            pltpu.VMEM((layers, TAIL, TAIL), jnp.int32),
            pltpu.VMEM((TOTAL, shards, group, span), BF16),
            pltpu.VMEM(fact, jnp.int32),
            pltpu.VMEM(fact, jnp.int32),
            pltpu.VMEM(fact, jnp.int32),
            pltpu.VMEM((TOTAL, shards, group, width + TAIL), F32),
            pltpu.VMEM((TOTAL, shards, group, width + TAIL), BF16),
            pltpu.VMEM((TOTAL, shards, group, width + TAIL), BF16),
            pltpu.VMEM((TOTAL, shards, group, query_width), BF16),
            dma((2 * layers + 1,)),
            dma((1,)),
            dma((SORTED, layers)),
            pltpu.SemaphoreType.REGULAR,
            dma((TOTAL, layers)),
            dma((TOTAL, shards - 1)),
            dma((TOTAL, shards)),
            dma((TOTAL, shards - 1)),
            dma((TOTAL, shards)),
            dma((TOTAL, layers)),
            dma((TOTAL,)),
        ],
        compiler_params=pltpu.CompilerParams(
            collective_id=1, has_side_effects=True, vmem_limit_bytes=56 << 20
        ),
    )(hidden, gain, proj_weight, out_weight, cache, exits, lens)


def body(hidden, exit_layer, lengths, kv_cache, norm_gain, w_qkv, w_out):
    devices = lax.axis_size("section")
    shards = max(2, devices // 4)
    layers = devices // shards
    tokens = exit_layer.shape[0]
    cache = kv_cache.reshape(kv_cache.shape[1] * kv_cache.shape[2], kv_cache.shape[3])
    exits = exit_layer.reshape(tokens // TAIL, TAIL)
    lens = lengths.reshape(tokens // TAIL, TAIL)
    operands = (hidden[0], norm_gain, w_qkv[0], w_out[0], cache, exits, lens)
    held = exit_layer.reshape(MICRO // layers, layers, shards, BLOCK // shards)

    def beyond(depth, first):
        deep = jnp.sum((held > depth).astype(jnp.int32), axis=(0, 3))
        return jnp.sum(jnp.maximum(deep - first, 0), axis=0)

    over = jnp.maximum(beyond(layers - 1, FIRST), beyond(1, KEEP))
    fits = jnp.max(over) <= BLOCK // shards // PARTS
    return lax.cond(
        fits,
        functools.partial(early, shards, layers),
        functools.partial(full, shards, layers),
        *operands,
    )


def solution(mesh):
    return jax.shard_map(
        body,
        mesh=mesh,
        in_specs=(
            P("section", "blk", None),
            P("blk"),
            P("blk"),
            P("section", "blk", None, None),
            P("section", None),
            P("section", None, None),
            P("section", None, None),
        ),
        out_specs=P("blk", "section"),
        check_vma=False,
    )
```

```python
import functools
import math

import jax
import jax.numpy as jnp
from jax import lax
from jax.experimental import pallas as pl
from jax.experimental.pallas import tpu as pltpu
from jax.sharding import PartitionSpec as P

BLOCK = 64
MICRO = 8
PARTS = 2
CHUNKS = MICRO * PARTS
CONTEXT = 16
SORTED = 4
FIRST = 8
KEEP = 16
POSITION = ((0, 1, 10, 11), (3, 7, 13, 16), (4, 8, 14, 17), (2, 6, 12, 15))
GATHERED = (5, 9)
WAITED = 15
DEEPEST = 6
DEEP = 10
TOTAL = 18
LAG_A = 1
LAG_U = 2
EPSILON = 1e-05
NEGATIVE = -1e30
TAIL = 128
MESH = pl.DeviceIdType.MESH
F32 = jnp.float32
BF16 = jnp.bfloat16


def full_kernel(
    shards,
    layers,
    hidden,
    gain,
    wq_hbm,
    wo_hbm,
    cache_hbm,
    exit_rows,
    length_rows,
    out,
    wq,
    wo,
    cache,
    inb,
    outb,
    exits,
    lens,
    accs,
    rs_send,
    rs_recv,
    att,
    w_sem,
    hid_ss,
    in_rs,
    rs_ss,
    rs_rs,
    ag_ss,
    ag_rs,
    st_ss,
    out_rs,
):
    me = lax.axis_index("section")
    y = me // shards
    x = me % shards
    last = layers - 1
    group, span = inb.shape[3:]
    rows = shards * group
    query_width = wo.shape[1]
    width = wq.shape[2]
    head = (width - query_width) // 2
    heads = query_width // head
    context = cache.shape[0] // (CHUNKS * group)
    total_width = span * shards * layers

    def remote(src, dst, send_sem, recv_sem, target):
        return pltpu.make_async_remote_copy(
            src_ref=src,
            dst_ref=dst,
            send_sem=send_sem,
            recv_sem=recv_sem,
            device_id={"section": target},
            device_id_type=MESH,
        )

    def row_peer(d):
        return y * shards + (x + d) % shards

    wq_copies = [
        pltpu.make_async_copy(wq_hbm.at[pl.ds(j * span, span)], wq.at[j], w_sem.at[j])
        for j in range(layers)
    ]
    wo_copies = [
        pltpu.make_async_copy(
            wo_hbm.at[:, pl.ds(j * span, span)], wo.at[j], w_sem.at[layers + j]
        )
        for j in range(layers)
    ]
    cache_copy = pltpu.make_async_copy(cache_hbm, cache, w_sem.at[2 * layers])
    for copy in wq_copies:
        copy.start()
    cache_copy.start()
    for copy in wo_copies:
        copy.start()

    barrier = pltpu.get_barrier_semaphore()
    for d in range(1, shards):
        pl.semaphore_signal(
            barrier, inc=1, device_id={"section": row_peer(d)}, device_id_type=MESH
        )
    for d in range(1, layers):
        pl.semaphore_signal(
            barrier,
            inc=1,
            device_id={"section": ((y + d) % layers) * shards + x},
            device_id_type=MESH,
        )
    pl.semaphore_wait(barrier, shards + layers - 2)

    rounds = MICRO // layers
    place = (layers - y) % layers

    pieces = [
        (q, h, j) for q in range(rounds) for h in range(PARTS) for j in range(layers)
    ]

    def hidden_piece(q, h, j):
        return hidden.at[q, :, h, :, pl.ds(j * span, span)]

    def hidden_copy(q, h, j):
        i = (q * layers + place) * PARTS + h
        return remote(
            hidden_piece(q, h, j), inb.at[i, j], hid_ss.at[q, h, j], in_rs.at[i, j], x
        )

    @pl.when(y == 0)
    def _():
        for q, h, j in pieces:
            i = q * layers * PARTS + h
            pltpu.make_async_copy(
                hidden_piece(q, h, j), inb.at[i, j], in_rs.at[i, j]
            ).start()

    @pl.when(y != 0)
    def _():
        for q, h, j in pieces:
            hidden_copy(q, h, j).start()

    for r in range(exit_rows.shape[0]):
        for source, target in ((exit_rows, exits), (length_rows, lens)):
            spread = jnp.broadcast_to(source[r : r + 1, :], (TAIL, TAIL)).T
            count = TAIL // BLOCK
            target[r * count : (r + 1) * count] = spread.reshape(
                (count,) + target.shape[1:]
            )

    def rs_copy(i, d):
        target = (x + d) % shards
        return remote(
            rs_send.at[i, target],
            rs_recv.at[i, x],
            rs_ss.at[i, d - 1],
            rs_rs.at[i, x],
            row_peer(d),
        )

    def rs_arrival(i, d):
        source = (x + d) % shards
        return remote(
            rs_send.at[i, source],
            rs_recv.at[i, source],
            rs_ss.at[i, d - 1],
            rs_rs.at[i, source],
            row_peer(d),
        )

    def ag_copy(i, d):
        return remote(
            att.at[i, x], att.at[i, x], ag_ss.at[i, d - 1], ag_rs.at[i, x], row_peer(d)
        )

    def ag_arrival(i, d):
        source = (x + d) % shards
        return remote(
            att.at[i, source],
            att.at[i, source],
            ag_ss.at[i, d - 1],
            ag_rs.at[i, source],
            row_peer(d),
        )

    def state_copy(i, j):
        return remote(
            outb.at[i, j],
            inb.at[i, j],
            st_ss.at[i, j],
            in_rs.at[i, j],
            (me + shards) % (shards * layers),
        )

    def tokens(ref, i):
        return ref.at[i // PARTS, :, i % PARTS]

    def result_copy(i, j):
        return remote(
            outb.at[i, j], tokens(out, i), st_ss.at[i, j], out_rs.at[i], j * shards + x
        )

    def project(i):
        squares = jnp.zeros((rows, TAIL), F32)
        acc = None
        for j in range(layers):

            @pl.when(i == 0)
            def _():
                wq_copies[j].wait()

            state_copy(i, j).wait_recv()
            state = inb[i, j].astype(F32).reshape(rows, span)
            scaled = (state * gain[:, pl.ds(j * span, span)].astype(F32)).astype(BF16)
            squared = state * state
            for n in range(span // TAIL):
                squares = squares + squared[:, n * TAIL : (n + 1) * TAIL]
            part = jnp.dot(scaled, wq[j], preferred_element_type=F32)
            acc = part if acc is None else acc + part
        total = jnp.sum(squares, axis=1, keepdims=True)
        coarse = total.astype(BF16).astype(F32)
        lane = lax.broadcasted_iota(jnp.int32, (rows, TAIL), 1)
        tail = jnp.where(lane < TAIL // 2, coarse, total - coarse)
        for g in range(shards):
            part = slice(g * group, (g + 1) * group)
            accs[i, g, :, :width] = acc[part]
            accs[i, g, :, width:] = tail[part]
            rs_send[i, g, :, :width] = acc[part].astype(BF16)
            rs_send[i, g, :, width:] = tail[part].astype(BF16)
        for d in (2, 1, 3):
            rs_copy(i, d).start()

    def attend(i):
        @pl.when(i == 0)
        def _():
            cache_copy.wait()

        summed = accs[i, x]
        for d in (1, 3, 2):
            rs_arrival(i, d).wait_recv()
        for d in (1, 3, 2):
            summed = summed + rs_recv[i, (x + d) % shards].astype(F32)
        squares = jnp.sum(summed[:, width:], axis=1, keepdims=True) * (2.0 / TAIL)
        scale = lax.rsqrt(squares / total_width + EPSILON)
        fitted = summed[:, :width] * scale
        query = fitted[:, :query_width] * (1.0 / math.sqrt(head))
        query = jnp.concatenate(
            [query[:, h * head : (h + 1) * head] for h in range(heads)], axis=0
        ).astype(BF16)
        key_new = fitted[:, query_width : query_width + head].astype(BF16).astype(F32)
        value_new = fitted[:, query_width + head :].astype(BF16).astype(F32)
        key_new = jnp.concatenate([key_new] * heads, axis=0)
        value_new = jnp.concatenate([value_new] * heads, axis=0)
        held = group * context
        keys = cache[pl.ds(pl.multiple_of(i * held, held), held), :head]
        values = cache[pl.ds(pl.multiple_of(i * held, held), held), head:]
        scores = lax.dot_general(
            query, keys, (((1,), (1,)), ((), ())), preferred_element_type=F32
        )
        own = jnp.sum(query.astype(F32) * key_new, axis=1, keepdims=True)
        reach = lens[i // PARTS, x, i % PARTS]
        reach = jnp.concatenate([reach] * (held // TAIL), axis=1)
        reach = jnp.concatenate([reach] * heads, axis=0)
        shape = (heads * group, held)
        row = lax.broadcasted_iota(jnp.int32, shape, 0)
        column = lax.broadcasted_iota(jnp.int32, shape, 1)
        offset = column - (row % group) * context
        usable = (offset >= 0) & (offset < reach)
        scores = jnp.where(usable, scores, NEGATIVE)
        top = jnp.maximum(jnp.max(scores, axis=1, keepdims=True), own)
        raw = jnp.where(usable, jnp.exp(scores - top), 0.0)
        raw_own = jnp.exp(own - top)
        total = jnp.sum(raw, axis=1, keepdims=True) + raw_own
        inverse = 1.0 / total
        weights = (raw * inverse).astype(BF16)
        own_weight = (raw_own * inverse).astype(BF16).astype(F32)
        attended = jnp.dot(weights, values, preferred_element_type=F32)
        attended = attended + own_weight * value_new
        att[i, x] = jnp.concatenate(
            [attended[h * group : (h + 1) * group] for h in range(heads)], axis=1
        ).astype(BF16)
        for d in (2, 1, 3):
            ag_copy(i, d).start()

    def update(i):
        for d in (1, 3, 2):
            ag_arrival(i, d).wait_recv()
        attended = att[i].astype(F32).reshape(rows, query_width).astype(BF16)
        depth = exits[i // PARTS, :, i % PARTS].reshape(rows, TAIL)
        active = jnp.concatenate([depth] * (span // TAIL), axis=1) > y
        for j in range(layers):

            @pl.when(i == 0)
            def _():
                wo_copies[j].wait()

            state = inb[i, j].astype(F32).reshape(rows, span)
            branch = jnp.dot(attended, wo[j], preferred_element_type=F32)
            updated = jnp.where(active, state + branch, state)
            updated = updated.reshape(shards, group, span).astype(BF16)
            outb[i, j] = updated

            @pl.when(y < last)
            def _():
                state_copy(i, j).start()

            if j < last:

                @pl.when(y == last)
                def _():
                    result_copy(i, j).start()

            else:

                @pl.when(y == last)
                def _():
                    out[i // PARTS, :, i % PARTS] = updated

    def step(i, carry):
        @pl.when(i < CHUNKS)
        def _():
            project(i)

        @pl.when((i >= LAG_A) & (i < CHUNKS + LAG_A))
        def _():
            attend(i - LAG_A)

        @pl.when(i >= LAG_U)
        def _():
            update(i - LAG_U)

        return carry

    lax.fori_loop(0, CHUNKS + LAG_U, step, 0)

    def finish(i, carry):
        for d in range(1, shards):
            rs_copy(i, d).wait_send()
            ag_copy(i, d).wait_send()
        for j in range(layers):

            @pl.when(y < last)
            def _():
                state_copy(i, j).wait_send()

            if j < last:

                @pl.when(y == last)
                def _():
                    result_copy(i, j).wait_send()

        @pl.when(y < last)
        def _():
            result_copy(i, 0).wait_recv()

        return carry

    lax.fori_loop(0, CHUNKS, finish, 0)

    @pl.when(y != 0)
    def _():
        for q, h, j in pieces:
            hidden_copy(q, h, j).wait_send()


def early_kernel(
    shards,
    layers,
    hidden,
    gain,
    wq_hbm,
    wo_hbm,
    cache_hbm,
    exit_rows,
    length_rows,
    out,
    wq,
    wo,
    cache,
    inb,
    outb,
    hid,
    staged,
    relay,
    late_pick,
    late_cache,
    target,
    settled,
    exits,
    lens,
    starts,
    accs,
    rs_send,
    rs_recv,
    att,
    w_sem,
    hid_in,
    hid_ss,
    turn,
    relay_ss,
    relay_rs,
    in_rs,
    rs_ss,
    rs_rs,
    ag_ss,
    ag_rs,
    st_ss,
    out_rs,
):
    me = lax.axis_index("section")
    y = me // shards
    x = me % shards
    last = layers - 1
    group, span = inb.shape[3:]
    rows = shards * group
    query_width = wo.shape[1]
    width = wq.shape[2]
    head = (width - query_width) // 2
    heads = query_width // head
    context = CONTEXT
    passing = DEEP - (DEEP - DEEPEST) * (y // (last - 1))
    count = (
        DEEP
        + (TOTAL - DEEP) * ((last - y) // last)
        - (DEEP - DEEPEST) * (y // last)
    )
    total_width = span * shards * layers

    def remote(src, dst, send_sem, recv_sem, target):
        return pltpu.make_async_remote_copy(
            src_ref=src,
            dst_ref=dst,
            send_sem=send_sem,
            recv_sem=recv_sem,
            device_id={"section": target},
            device_id_type=MESH,
        )

    def row_peer(d):
        return y * shards + (x + d) % shards

    wq_copies = [
        pltpu.make_async_copy(wq_hbm.at[pl.ds(j * span, span)], wq.at[j], w_sem.at[j])
        for j in range(layers)
    ]
    wo_copies = [
        pltpu.make_async_copy(
            wo_hbm.at[:, pl.ds(j * span, span)], wo.at[j], w_sem.at[layers + j]
        )
        for j in range(layers)
    ]
    cache_copy = pltpu.make_async_copy(cache_hbm, cache, w_sem.at[2 * layers])
    hid_copy = pltpu.make_async_copy(hidden, hid, hid_in.at[0])
    hid_copy.start()
    for copy in wq_copies:
        copy.start()
    cache_copy.start()
    for copy in wo_copies:
        copy.start()

    barrier = pltpu.get_barrier_semaphore()
    for d in range(1, shards):
        pl.semaphore_signal(
            barrier, inc=1, device_id={"section": row_peer(d)}, device_id_type=MESH
        )
    for d in range(1, layers):
        pl.semaphore_signal(
            barrier,
            inc=1,
            device_id={"section": ((y + d) % layers) * shards + x},
            device_id_type=MESH,
        )

    wide = (TAIL, TAIL)
    t0 = lax.broadcasted_iota(jnp.int32, wide, 0)
    t1 = lax.broadcasted_iota(jnp.int32, wide, 1)
    g0 = (t0 & (BLOCK - 1)) >> 4
    g1 = (t1 & (BLOCK - 1)) >> 4
    same = g0 == g1
    lane_group = (t1 & 31) >> 3
    lane_rank = ((t1 >> 5) << 3) + (t1 & 7)
    slot_row = lax.broadcasted_iota(jnp.int32, (rows, TAIL), 0)
    low_half = t1 < BLOCK
    def number(mask):
        return jnp.where(mask, 1.0, 0.0)

    def piece_row(ref, p):
        first = jnp.broadcast_to(ref[pl.ds(p // 2, 1), :], wide)
        second = jnp.broadcast_to(ref[pl.ds(p // 2 + 2, 1), :], wide)
        even = jnp.where(low_half, first, pltpu.roll(second, BLOCK, 1))
        odd = jnp.where(low_half, pltpu.roll(first, BLOCK, 1), second)
        if isinstance(p, int):
            return odd if p % 2 else even
        parity = p % 2
        return even * (1 - parity) + odd * parity

    def rank_of(exit_row, exit_column):
        ahead = same & (
            (exit_column > exit_row) | ((exit_column == exit_row) & (t0 < t1))
        )
        rank_lane = jnp.sum(number(ahead), axis=0, keepdims=True).astype(jnp.int32)
        order_lane = ((rank_lane >> 3) << 5) + (g1 << 3) + (rank_lane & 7)
        return number(order_lane == t0).astype(BF16)

    own_row = piece_row(exit_rows, (layers - y) % layers)
    own_pick = rank_of(own_row, own_row.T)

    hid_copy.wait()
    for j in range(layers):
        ordered = jnp.dot(
            own_pick,
            hid[:, j * span : (j + 1) * span],
            preferred_element_type=F32,
        )
        ordered = ordered.reshape(SORTED, shards, group, span).astype(BF16)

        @pl.when(y == 0)
        def _():
            for c in range(SORTED):
                inb[POSITION[0][c], j] = ordered[c]

        @pl.when(y != 0)
        def _():
            for c in range(SORTED):
                staged[c, j] = ordered[c]

    pl.semaphore_wait(barrier, shards + layers - 2)

    def hidden_copy(p, c, j):
        i = POSITION[p][c]
        return remote(
            staged.at[c, j], inb.at[i, j], hid_ss.at[c, j], in_rs.at[i, j], x
        )

    def hidden_start(p, c):
        for j in range(layers):
            hidden_copy(p, c, j).start()

    def hidden_sent(p, c, pieces):
        for j in pieces:
            hidden_copy(p, c, j).wait_send()

    every = range(layers)

    def next_turn():
        pl.semaphore_signal(
            turn, inc=1, device_id={"section": me - shards}, device_id_type=MESH
        )

    def relay_copy(j):
        return remote(
            staged.at[1, j], relay.at[j], hid_ss.at[1, j], relay_rs.at[j], shards + x
        )

    def relay_on(j):
        i = POSITION[2][1]
        return remote(relay.at[j], inb.at[i, j], relay_ss.at[j], in_rs.at[i, j], x)

    @pl.when(y == 1)
    def _():
        for c in range(2):
            hidden_start(3, c)
            hidden_sent(3, c, every)
        for j in every:
            relay_copy(j).wait_recv()
            relay_on(j).start()
        for c in range(2, SORTED):
            hidden_start(3, c)

    @pl.when(y == 2)
    def _():
        for j in every:
            relay_copy(j).start()
        for c in (0, 2, 3):
            pl.semaphore_wait(turn, 1)
            hidden_start(2, c)

    @pl.when(y == 3)
    def _():
        hidden_start(1, 0)
        hidden_sent(1, 0, every[:2])
        next_turn()
        hidden_sent(1, 0, every[2:])
        for c in (1, 2):
            hidden_start(1, c)
            hidden_sent(1, c, every)
            next_turn()
        hidden_start(1, 3)

    def prepare():
        kinds = ((FIRST, last), (KEEP, 1))
        base_lane = [jnp.zeros((1, TAIL), jnp.int32) for _ in kinds]
        base_column = [jnp.zeros((TAIL, 1), jnp.int32) for _ in kinds]
        late = [jnp.zeros((rows, 3 * TAIL), F32) for _ in kinds]

        for p in range(layers):
            exit_row = piece_row(exit_rows, p)
            exit_column = exit_row.T
            length_column = piece_row(length_rows, p).T
            pick = rank_of(exit_row, exit_column)
            behind = same & (
                (exit_row > exit_column) | ((exit_row == exit_column) & (t1 < t0))
            )
            rank_column = jnp.sum(number(behind), axis=1, keepdims=True).astype(jnp.int32)
            order_column = ((rank_column >> 3) << 5) + (g0 << 3) + (rank_column & 7)
            natural = ((p + layers * (t0 >> 6)) << 4) + (t0 & 15)
            facts = jnp.concatenate([exit_column, length_column, natural], axis=1)
            sorted_facts = jnp.dot(
                pick, facts.astype(F32).astype(BF16), preferred_element_type=F32
            )
            for c in range(SORTED):
                block = sorted_facts[c * rows : (c + 1) * rows].astype(jnp.int32)
                block = block.reshape(shards, group, 3 * TAIL)
                exits[POSITION[p][c]] = block[:, :, :TAIL]
                lens[POSITION[p][c]] = block[:, :, TAIL : 2 * TAIL]
                starts[POSITION[p][c]] = block[:, :, 2 * TAIL :] * context
            goal = order_column
            for n, (first, depth) in reversed(list(enumerate(kinds))):
                deep_column = jnp.sum(
                    number(same & (exit_row > depth)), axis=1, keepdims=True
                ).astype(jnp.int32)
                deep_lane = jnp.sum(
                    number((exit_column > depth) & (g0 == lane_group)), axis=0, keepdims=True
                ).astype(jnp.int32)
                ranked = lane_rank[:rows]
                chosen = (
                    (ranked >= first)
                    & (ranked < deep_lane)
                    & (lane_group[:rows] == (slot_row >> 3))
                    & (base_lane[n] + ranked - first == (slot_row & 7))
                )
                chosen = number(chosen).astype(BF16)
                late_pick[n, p] = chosen
                late[n] = late[n] + jnp.dot(
                    chosen, sorted_facts.astype(BF16), preferred_element_type=F32
                )
                goal = jnp.where(
                    (rank_column >= first) & (rank_column < deep_column),
                    TAIL + n * rows + (g0 << 3) + base_column[n] + rank_column - first,
                    goal,
                )
                base_lane[n] = base_lane[n] + jnp.maximum(deep_lane - first, 0)
                base_column[n] = base_column[n] + jnp.maximum(deep_column - first, 0)
            target[p] = goal
        for n, i in enumerate(GATHERED):
            block = late[n].astype(jnp.int32).reshape(shards, group, 3 * TAIL)
            exits[i] = block[:, :, :TAIL]
            lens[i] = block[:, :, TAIL : 2 * TAIL]
            starts[i] = block[:, :, 2 * TAIL :] * context
        cache_copy.wait()
        for n, i in enumerate(GATHERED):
            source = jnp.broadcast_to(
                starts[i, x].reshape(group, 1, TAIL), (group, context, TAIL)
            ).reshape(group * context, TAIL)
            source = source + lax.broadcasted_iota(jnp.int32, source.shape, 0) % context
            lane = lax.broadcasted_iota(jnp.int32, source.shape, 1)
            pick = [
                number(source == lane + m * TAIL).astype(BF16)
                for m in range(cache.shape[0] // TAIL)
            ]
            late_cache[n] = jnp.dot(
                jnp.concatenate(pick, axis=1), cache[...], preferred_element_type=F32
            ).astype(BF16)

    def rs_copy(i, d):
        target = (x + d) % shards
        return remote(
            rs_send.at[i, target],
            rs_recv.at[i, x],
            rs_ss.at[i, d - 1],
            rs_rs.at[i, x],
            row_peer(d),
        )

    def rs_arrival(i, d):
        source = (x + d) % shards
        return remote(
            rs_send.at[i, source],
            rs_recv.at[i, source],
            rs_ss.at[i, d - 1],
            rs_rs.at[i, source],
            row_peer(d),
        )

    def ag_copy(i, d):
        return remote(
            att.at[i, x], att.at[i, x], ag_ss.at[i, d - 1], ag_rs.at[i, x], row_peer(d)
        )

    def ag_arrival(i, d):
        source = (x + d) % shards
        return remote(
            att.at[i, source],
            att.at[i, source],
            ag_ss.at[i, d - 1],
            ag_rs.at[i, source],
            row_peer(d),
        )

    def state_copy(i, j):
        return remote(
            outb.at[i, j],
            inb.at[i, j],
            st_ss.at[i, j],
            in_rs.at[i, j],
            (me + shards) % (shards * layers),
        )

    def result_copy(i, j):
        return remote(
            outb.at[i, j], settled.at[i], st_ss.at[i, j], out_rs.at[i], j * shards + x
        )

    def gather_late(n, chunks):
        for c in chunks:
            for p in range(1, layers):
                for j in range(layers):
                    state_copy(POSITION[p][c], j).wait_recv()
        for j in range(layers):
            found = None
            for p in range(layers):
                held = [
                    inb[POSITION[p][c], j].astype(F32).reshape(rows, span)
                    if c in chunks
                    else jnp.zeros((rows, span), F32)
                    for c in range(SORTED)
                ]
                held = jnp.concatenate(held, axis=0).astype(BF16)
                part = jnp.dot(late_pick[n, p], held, preferred_element_type=F32)
                found = part if found is None else found + part
            inb[GATHERED[n], j] = found.reshape(shards, group, span).astype(BF16)

    def project(i):
        squares = jnp.zeros((rows, TAIL), F32)
        acc = None
        for j in range(layers):

            @pl.when(i == 0)
            def _():
                wq_copies[j].wait()

            @pl.when((y > 0) | ((i > 1) & (i < GATHERED[0])) | (i >= WAITED))
            def _():
                state_copy(i, j).wait_recv()

            state = inb[i, j].astype(F32).reshape(rows, span)
            scaled = (state * gain[:, pl.ds(j * span, span)].astype(F32)).astype(BF16)
            squared = state * state
            for n in range(span // TAIL):
                squares = squares + squared[:, n * TAIL : (n + 1) * TAIL]
            part = jnp.dot(scaled, wq[j], preferred_element_type=F32)
            acc = part if acc is None else acc + part
        total = jnp.sum(squares, axis=1, keepdims=True)
        coarse = total.astype(BF16).astype(F32)
        lane = lax.broadcasted_iota(jnp.int32, (rows, TAIL), 1)
        tail = jnp.where(lane < TAIL // 2, coarse, total - coarse)
        for g in range(shards):
            part = slice(g * group, (g + 1) * group)
            accs[i, g, :, :width] = acc[part]
            accs[i, g, :, width:] = tail[part]
            rs_send[i, g, :, :width] = acc[part].astype(BF16)
            rs_send[i, g, :, width:] = tail[part].astype(BF16)
        for d in (2, 1, 3):
            rs_copy(i, d).start()

    def attend(i):
        turn = (1 - i // DEEP) * ((i + 2) % layers) + (i // DEEP) * (i % last)
        p = ((i % DEEP + 8) // DEEP) * ((last - 2 * turn + last * (turn // 2)) % layers)
        half = shards * shards * context
        lane = lax.broadcasted_iota(jnp.int32, (heads * group, TAIL), 1)

        @pl.when((i == GATHERED[0]) | (i == GATHERED[1]))
        def _():
            n = i // GATHERED[1]
            row = lax.broadcasted_iota(jnp.int32, (heads * group, TAIL), 0)
            attend_over(
                i,
                late_cache[n, :, :head],
                late_cache[n, :, head:],
                [lane - (row % group) * context],
            )

        @pl.when((i != GATHERED[0]) & (i != GATHERED[1]))
        def _():
            pieces = [pl.multiple_of(m * half, half) for m in (p, p + layers)]
            start = jnp.concatenate([starts[i, x]] * heads, axis=0)
            attend_over(
                i,
                jnp.concatenate([cache[pl.ds(at, half), :head] for at in pieces], axis=0),
                jnp.concatenate([cache[pl.ds(at, half), head:] for at in pieces], axis=0),
                [
                    lane + (at + m * TAIL) - start
                    for at in pieces
                    for m in range(half // TAIL)
                ],
            )

    def attend_over(i, keys, values, offset):

        summed = accs[i, x]
        for d in (1, 3, 2):
            rs_arrival(i, d).wait_recv()
        for d in (1, 3, 2):
            summed = summed + rs_recv[i, (x + d) % shards].astype(F32)
        squares = jnp.sum(summed[:, width:], axis=1, keepdims=True) * (2.0 / TAIL)
        scale = lax.rsqrt(squares / total_width + EPSILON)
        fitted = summed[:, :width] * scale
        query = fitted[:, :query_width] * (1.0 / math.sqrt(head))
        query = jnp.concatenate(
            [query[:, h * head : (h + 1) * head] for h in range(heads)], axis=0
        ).astype(BF16)
        key_new = fitted[:, query_width : query_width + head].astype(BF16).astype(F32)
        value_new = fitted[:, query_width + head :].astype(BF16).astype(F32)
        key_new = jnp.concatenate([key_new] * heads, axis=0)
        value_new = jnp.concatenate([value_new] * heads, axis=0)
        scores = lax.dot_general(
            query, keys, (((1,), (1,)), ((), ())), preferred_element_type=F32
        )
        own = jnp.sum(query.astype(F32) * key_new, axis=1, keepdims=True)
        reach = jnp.concatenate([lens[i, x]] * heads, axis=0)
        reach = jnp.concatenate([reach] * len(offset), axis=1)
        offset = jnp.concatenate(offset, axis=1)
        usable = (offset >= 0) & (offset < reach)
        scores = jnp.where(usable, scores, NEGATIVE)
        top = jnp.maximum(jnp.max(scores, axis=1, keepdims=True), own)
        raw = jnp.where(usable, jnp.exp(scores - top), 0.0)
        raw_own = jnp.exp(own - top)
        total = jnp.sum(raw, axis=1, keepdims=True) + raw_own
        inverse = 1.0 / total
        weights = (raw * inverse).astype(BF16)
        own_weight = (raw_own * inverse).astype(BF16).astype(F32)
        attended = jnp.dot(weights, values, preferred_element_type=F32)
        attended = attended + own_weight * value_new
        att[i, x] = jnp.concatenate(
            [attended[h * group : (h + 1) * group] for h in range(heads)], axis=1
        ).astype(BF16)
        for d in (2, 1, 3):
            ag_copy(i, d).start()

    def update(i):
        for d in (1, 3, 2):
            ag_arrival(i, d).wait_recv()
        attended = att[i].astype(F32).reshape(rows, query_width).astype(BF16)
        depth = exits[i].reshape(rows, TAIL)
        final = (y == last) | (i >= passing)
        active = jnp.concatenate([depth] * (span // TAIL), axis=1) > y
        for j in range(layers):

            @pl.when(i == 0)
            def _():
                wo_copies[j].wait()

            state = inb[i, j].astype(F32).reshape(rows, span)
            branch = jnp.dot(attended, wo[j], preferred_element_type=F32)
            updated = jnp.where(active, state + branch, state)
            updated = updated.reshape(shards, group, span).astype(BF16)
            outb[i, j] = updated

            @pl.when((y < last) & (i < passing))
            def _():
                state_copy(i, j).start()

            @pl.when(final & (y != j))
            def _():
                result_copy(i, j).start()

            @pl.when(final & (y == j))
            def _():
                settled[i] = updated

    def step(i, carry):
        @pl.when((y == 0) & (i == GATHERED[0]))
        def _():
            gather_late(0, (1,))

        @pl.when((y == 0) & (i == GATHERED[1]))
        def _():
            gather_late(1, (2,))

        @pl.when(i < count)
        def _():
            project(i)

        @pl.when(i == LAG_A)
        def _():
            prepare()

        behind = i - LAG_A - LAG_A * (i // (DEEP + LAG_A))

        @pl.when(
            (i >= LAG_A)
            & ((i < DEEP + LAG_A) | (i >= DEEP + 2 * LAG_A))
            & (behind < count)
        )
        def _():
            attend(behind)

        far_behind = i - LAG_U - LAG_U * (i // (DEEP + LAG_U))

        @pl.when(
            (i >= LAG_U)
            & ((i < DEEP + LAG_U) | (i >= DEEP + 2 * LAG_U))
            & (far_behind < count)
        )
        def _():
            update(far_behind)

        return carry

    lax.fori_loop(0, count + LAG_U + LAG_U * ((last - y) // last), step, 0)

    def arrive(i, carry):
        @pl.when(
            ((y != last) & (i < DEEPEST))
            | ((y != last - 1) & (i >= DEEPEST) & (i < DEEP))
            | ((y != 0) & (i >= DEEP))
        )
        def _():
            result_copy(i, 0).wait_recv()

        return carry

    lax.fori_loop(0, TOTAL, arrive, 0)

    reach = lax.broadcasted_iota(jnp.int32, wide, 1)
    extra = [settled[i].astype(F32).reshape(rows, span) for i in GATHERED]
    extra = jnp.concatenate(extra + [jnp.zeros((2 * rows, span), F32)], axis=0)
    extra = extra.astype(BF16)
    for p in range(layers):
        found = jnp.concatenate(
            [
                settled[POSITION[p][c]].astype(F32).reshape(rows, span)
                for c in range(SORTED)
            ],
            axis=0,
        ).astype(BF16)
        goal = target[p]
        result = jnp.dot(
            number(goal == reach).astype(BF16), found, preferred_element_type=F32
        ) + jnp.dot(
            number(goal == reach + TAIL).astype(BF16), extra, preferred_element_type=F32
        )
        result = result.astype(BF16)
        out[p * BLOCK : (p + 1) * BLOCK, :] = result[:BLOCK]
        out[(p + layers) * BLOCK : (p + layers + 1) * BLOCK, :] = result[BLOCK:]

    def finish(i, carry):
        for d in range(1, shards):
            rs_copy(i, d).wait_send()
            ag_copy(i, d).wait_send()
        final = (y == last) | (i >= passing)
        for j in range(layers):

            @pl.when((y < last) & (i < passing))
            def _():
                state_copy(i, j).wait_send()

            @pl.when(final & (y != j))
            def _():
                result_copy(i, j).wait_send()

        return carry

    lax.fori_loop(0, count, finish, 0)

    @pl.when(y == 1)
    def _():
        for c in range(2, SORTED):
            hidden_sent(3, c, every)
        for j in every:
            relay_on(j).wait_send()

    @pl.when(y == 2)
    def _():
        for j in every:
            relay_copy(j).wait_send()
        for c in (0, 2, 3):
            hidden_sent(2, c, every)

    @pl.when(y == 3)
    def _():
        hidden_sent(1, 3, every)


def full(shards, layers, hidden, gain, proj_weight, out_weight, cache, exits, lens):
    tokens = exits.shape[0] * exits.shape[1]
    quarter, width = proj_weight.shape
    query_width = out_weight.shape[0]
    span = quarter // layers
    group = BLOCK // shards // PARTS
    hidden = hidden.reshape(MICRO // layers, shards, PARTS, group, quarter)
    anywhere = pl.BlockSpec(memory_space=pl.ANY)
    vmem = pl.BlockSpec(memory_space=pltpu.VMEM)
    dma = pltpu.SemaphoreType.DMA
    column = (MICRO, shards, PARTS, group, TAIL)
    settled = pl.pallas_call(
        functools.partial(full_kernel, shards, layers),
        out_shape=jax.ShapeDtypeStruct((MICRO, shards, PARTS, group, span), BF16),
        in_specs=[anywhere, vmem, anywhere, anywhere, anywhere, vmem, vmem],
        out_specs=vmem,
        scratch_shapes=[
            pltpu.VMEM((layers, span, width), BF16),
            pltpu.VMEM((layers, query_width, span), BF16),
            pltpu.VMEM(cache.shape, BF16),
            pltpu.VMEM((CHUNKS, layers, shards, group, span), BF16),
            pltpu.VMEM((CHUNKS, layers, shards, group, span), BF16),
            pltpu.VMEM(column, jnp.int32),
            pltpu.VMEM(column, jnp.int32),
            pltpu.VMEM((CHUNKS, shards, group, width + TAIL), F32),
            pltpu.VMEM((CHUNKS, shards, group, width + TAIL), BF16),
            pltpu.VMEM((CHUNKS, shards, group, width + TAIL), BF16),
            pltpu.VMEM((CHUNKS, shards, group, query_width), BF16),
            dma((2 * layers + 1,)),
            dma((MICRO // layers, PARTS, layers)),
            dma((CHUNKS, layers)),
            dma((CHUNKS, shards - 1)),
            dma((CHUNKS, shards)),
            dma((CHUNKS, shards - 1)),
            dma((CHUNKS, shards)),
            dma((CHUNKS, layers)),
            dma((CHUNKS,)),
        ],
        compiler_params=pltpu.CompilerParams(
            collective_id=0, has_side_effects=True, vmem_limit_bytes=56 << 20
        ),
    )(hidden, gain, proj_weight, out_weight, cache, exits, lens)
    return settled.reshape(tokens, span)


def early(shards, layers, hidden, gain, proj_weight, out_weight, cache, exits, lens):
    tokens = exits.shape[0] * exits.shape[1]
    quarter, width = proj_weight.shape
    query_width = out_weight.shape[0]
    span = quarter // layers
    group = BLOCK // shards // PARTS
    rows = shards * group
    anywhere = pl.BlockSpec(memory_space=pl.ANY)
    vmem = pl.BlockSpec(memory_space=pltpu.VMEM)
    dma = pltpu.SemaphoreType.DMA
    fact = (TOTAL, shards, group, TAIL)
    return pl.pallas_call(
        functools.partial(early_kernel, shards, layers),
        out_shape=jax.ShapeDtypeStruct((tokens, span), BF16),
        in_specs=[anywhere, vmem, anywhere, anywhere, anywhere, vmem, vmem],
        out_specs=vmem,
        scratch_shapes=[
            pltpu.VMEM((layers, span, width), BF16),
            pltpu.VMEM((layers, query_width, span), BF16),
            pltpu.VMEM(cache.shape, BF16),
            pltpu.VMEM((TOTAL, layers, shards, group, span), BF16),
            pltpu.VMEM((TOTAL, layers, shards, group, span), BF16),
            pltpu.VMEM(hidden.shape, BF16),
            pltpu.VMEM((SORTED, layers, shards, group, span), BF16),
            pltpu.VMEM((layers, shards, group, span), BF16),
            pltpu.VMEM((2, layers, rows, TAIL), BF16),
            pltpu.VMEM((2, group * CONTEXT, cache.shape[1]), BF16),
            pltpu.VMEM((layers, TAIL, TAIL), jnp.int32),
            pltpu.VMEM((TOTAL, shards, group, span), BF16),
            pltpu.VMEM(fact, jnp.int32),
            pltpu.VMEM(fact, jnp.int32),
            pltpu.VMEM(fact, jnp.int32),
            pltpu.VMEM((TOTAL, shards, group, width + TAIL), F32),
            pltpu.VMEM((TOTAL, shards, group, width + TAIL), BF16),
            pltpu.VMEM((TOTAL, shards, group, width + TAIL), BF16),
            pltpu.VMEM((TOTAL, shards, group, query_width), BF16),
            dma((2 * layers + 1,)),
            dma((1,)),
            dma((SORTED, layers)),
            pltpu.SemaphoreType.REGULAR,
            dma((layers,)),
            dma((layers,)),
            dma((TOTAL, layers)),
            dma((TOTAL, shards - 1)),
            dma((TOTAL, shards)),
            dma((TOTAL, shards - 1)),
            dma((TOTAL, shards)),
            dma((TOTAL, layers)),
            dma((TOTAL,)),
        ],
        compiler_params=pltpu.CompilerParams(
            collective_id=1, has_side_effects=True, vmem_limit_bytes=56 << 20
        ),
    )(hidden, gain, proj_weight, out_weight, cache, exits, lens)


def body(hidden, exit_layer, lengths, kv_cache, norm_gain, w_qkv, w_out):
    devices = lax.axis_size("section")
    shards = max(2, devices // 4)
    layers = devices // shards
    tokens = exit_layer.shape[0]
    cache = kv_cache.reshape(kv_cache.shape[1] * kv_cache.shape[2], kv_cache.shape[3])
    exits = exit_layer.reshape(tokens // TAIL, TAIL)
    lens = lengths.reshape(tokens // TAIL, TAIL)
    operands = (hidden[0], norm_gain, w_qkv[0], w_out[0], cache, exits, lens)
    held = exit_layer.reshape(MICRO // layers, layers, shards, BLOCK // shards)

    def beyond(depth, first):
        deep = jnp.sum((held > depth).astype(jnp.int32), axis=(0, 3))
        return jnp.sum(jnp.maximum(deep - first, 0), axis=0)

    over = jnp.maximum(beyond(layers - 1, FIRST), beyond(1, KEEP))
    fits = jnp.max(over) <= BLOCK // shards // PARTS
    return lax.cond(
        fits,
        functools.partial(early, shards, layers),
        functools.partial(full, shards, layers),
        *operands,
    )


def solution(mesh):
    return jax.shard_map(
        body,
        mesh=mesh,
        in_specs=(
            P("section", "blk", None),
            P("blk"),
            P("blk"),
            P("section", "blk", None, None),
            P("section", None),
            P("section", None, None),
            P("section", None, None),
        ),
        out_specs=P("blk", "section"),
        check_vma=False,
    )
```
